256 devices in a mesh: outer: 4 (over x), inner: 64 (over z, y, core).
Axes of the slice: x: 4, y: 4, z: 8, core: 2. Of those that a mesh axis runs over, the one named last changes fastest.
Arguments:
- prim: float32 [8, 3072, 512], P(None, ('outer', 'inner')), may hold values from -4 to 9, as said below
- new_owner: int32 [3072], replicated, may hold values from 0 to 255, as said below
- new_slot: int32 [3072], replicated, may hold values from 0 to 23, as said below
Outputs:
- placed: float32 [8, 6144, 512], P(None, ('outer', 'inner'))
The draws below stay inside these ranges and needn't reach their ends.
Inputs may be any that keep to these rules, and one draw needn't show every extreme that they name: `prim`: field 0 (density) lies in 0.3 to 3 and field 4 (pressure) in 0.2 to 9; fields 1 to 3 are velocities and 5 to 7 the magnetic field. `new_owner`: block g's owner lies in the segment of 64 devices that holds device g // 12 and differs from g // 12 by at most one; owners never fall along g, so every device gets a run of consecutive blocks (possibly none); at most 6 blocks of one device go to each neighbour, and in every draw some device of each segment receives 24 blocks. `new_slot`: the blocks of one owner have slots 0, 1, 2, ... in the order of g.
All inputs are finite; a program needn't handle non-finite values.
Results may differ from the reference program's by a relative error of at most 0.0003.
Values sent between devices are 32-bit elements; how exact they have to be, the bound alone decides.
No kernel may reach another device: no remote copies, remote signals or barrier semaphores. Data moves between devices by JAX's collectives and lax.ppermute only.
A program may use at most 64 MiB of HBM per device.

```python
import math
import jax
import jax.numpy as jnp
from jax import lax

BE = 8
GY = 16
BLK_DEV = 12
MOVE = 6
CAP = 24
CELLS = 512
NBLK = 3072
SEGMENTS = 4
RANKS = 64


def assignment(key):
    base = jax.random.fold_in(key, 7)
    shift_key, pick_key = jax.random.split(base)
    offsets = jax.random.randint(shift_key, (SEGMENTS, RANKS), -MOVE, MOVE + 1)
    chosen = jax.random.randint(pick_key, (SEGMENTS, 1), 1, RANKS - 1)
    ranks_row = jnp.arange(RANKS, dtype=jnp.int32)[None, :]
    offsets = jnp.where(ranks_row == chosen, -MOVE, offsets)
    offsets = jnp.where(ranks_row == chosen + 1, MOVE, offsets)
    offsets = jnp.where(ranks_row == 0, 0, offsets)
    starts = BLK_DEV * ranks_row + offsets
    local_ids = jnp.arange(RANKS * BLK_DEV, dtype=jnp.int32)
    owner_local = jnp.sum((starts[:, None, :] <= local_ids[None, :, None]).astype(jnp.int32), axis=2) - 1
    start_of = jnp.take_along_axis(starts, owner_local, axis=1)
    slot_ids = local_ids[None, :] - start_of
    owners = owner_local + RANKS * jnp.arange(SEGMENTS, dtype=jnp.int32)[:, None]
    return (owners.reshape(-1).astype(jnp.int32), slot_ids.reshape(-1).astype(jnp.int32))


def draw_new_owner(key, part):
    return assignment(key)[0]


def draw_new_slot(key, part):
    return assignment(key)[1]


def draw_prim(key, part):
    keys = jax.random.split(jax.random.fold_in(key, 31), 4)
    shape = (NBLK, CELLS)
    position = jnp.arange(NBLK, dtype=jnp.float32)[:, None] / max(NBLK - 1, 1)
    density = jnp.exp(jax.random.uniform(keys[0], shape, jnp.float32, math.log(0.5), math.log(2.0)))
    velocity = jnp.clip(0.5 * jax.random.normal(keys[1], (3,) + shape, jnp.float32), -3.0, 3.0)
    pressure = jnp.exp(jax.random.uniform(keys[2], shape, jnp.float32, math.log(0.2), math.log(1.0))) * (1.0 + 2.0 * position)
    magnetic = jnp.clip(0.7 * jax.random.normal(keys[3], (3,) + shape, jnp.float32), -4.0, 4.0)
    return jnp.concatenate([density[None], velocity, pressure[None], magnetic], 0).astype(jnp.float32)


def setup_inputs(seed: int = 0) -> dict:
    splits = jax.random.split(jax.random.key(seed), 4)
    return {
        "prim": draw_prim(jax.random.fold_in(splits[3], 71), 0),
        "new_owner": draw_new_owner(jax.random.fold_in(splits[3], 71), 0),
        "new_slot": draw_new_slot(jax.random.fold_in(splits[3], 71), 0),
    }


GAMMA = 5.0 / 3.0
COURANT = 0.8

def minmod(former, latter):
    return 0.5 * (jnp.sign(former) + jnp.sign(latter)) * jnp.minimum(jnp.abs(former), jnp.abs(latter))

def unpack(state):
    return [state[component] for component in range(8)]

def conserved(state):
    density, speed_x, speed_y, speed_z, pressure, field_x, field_y, field_z = unpack(state)
    kinetic = 0.5 * density * (speed_x * speed_x + speed_y * speed_y + speed_z * speed_z)
    magnetic = 0.5 * (field_x * field_x + field_y * field_y + field_z * field_z)
    energy = pressure / (GAMMA - 1.0) + kinetic + magnetic
    return jnp.stack([density, density * speed_x, density * speed_y, density * speed_z, energy, field_x, field_y, field_z])

def signal(state):
    density, speed_x, speed_y, speed_z, pressure, field_x, field_y, field_z = unpack(state)
    field_sq = field_x * field_x + field_y * field_y + field_z * field_z
    return jnp.abs(speed_x) + jnp.abs(speed_y) + jnp.abs(speed_z) + 3.0 * jnp.sqrt((GAMMA * pressure + field_sq) / density)

def flux_parts(state, normal):
    density, speed_x, speed_y, speed_z, pressure, field_x, field_y, field_z = unpack(state)
    velocity = (speed_x, speed_y, speed_z)
    magnetic = (field_x, field_y, field_z)
    normal_speed = velocity[normal]
    normal_field = magnetic[normal]
    field_sq = field_x * field_x + field_y * field_y + field_z * field_z
    total_pressure = pressure + 0.5 * field_sq
    conserved_state = conserved(state)
    vel_dot_field = speed_x * field_x + speed_y * field_y + speed_z * field_z
    momentum = []
    for component in range(3):
        momentum_term = density * velocity[component] * normal_speed - magnetic[component] * normal_field
        if component == normal:
            momentum_term = momentum_term + total_pressure
        momentum.append(momentum_term)
    induction = [magnetic[component] * normal_speed - velocity[component] * normal_field for component in range(3)]
    energy_flux = (conserved_state[4] + total_pressure) * normal_speed - normal_field * vel_dot_field
    flux_terms = jnp.stack([density * normal_speed] + momentum + [energy_flux] + induction)
    signal_speed = jnp.abs(normal_speed) + jnp.sqrt((GAMMA * pressure + field_sq) / density)
    return (flux_terms, signal_speed, conserved_state)

def divergence(padded, normal):
    cell_axis = normal + 1
    inner_count = padded.shape[cell_axis] - 4

    def window(values, offset, length):
        return lax.slice_in_dim(values, offset, offset + length, axis=cell_axis)
    steps_between = window(padded, 1, inner_count + 3) - window(padded, 0, inner_count + 3)
    slopes = minmod(window(steps_between, 0, inner_count + 2), window(steps_between, 1, inner_count + 2))
    centres = window(padded, 1, inner_count + 2)
    left_state = window(centres, 0, inner_count + 1) + 0.5 * window(slopes, 0, inner_count + 1)
    right_state = window(centres, 1, inner_count + 1) - 0.5 * window(slopes, 1, inner_count + 1)
    flux_left, speed_left, state_left = flux_parts(left_state, normal)
    flux_right, speed_right, state_right = flux_parts(right_state, normal)
    face_flux = 0.5 * (flux_left + flux_right) - 0.5 * jnp.maximum(speed_left, speed_right)[None] * (state_right - state_left)
    return window(face_flux, 1, inner_count) - window(face_flux, 0, inner_count)

def advance(x_padded, y_padded, z_padded, time_step):
    middle = x_padded[:, 2:-2]
    change = divergence(x_padded, 0) + divergence(y_padded, 1) + divergence(z_padded, 2)
    return conserved(middle) - time_step * change

def pencil_of(prim, device):
    edge_len = BE
    blocks_here = lax.dynamic_slice_in_dim(prim, (device * BLK_DEV).astype(jnp.int32), BLK_DEV, 1)
    shaped = blocks_here.reshape(8, BLK_DEV, edge_len, edge_len, edge_len).transpose(0, 2, 3, 1, 4)
    return shaped.reshape(8, edge_len, edge_len, BLK_DEV * edge_len)

def reference(prim, new_owner, new_slot):
    edge_len = BE
    devices_all = prim.shape[1] // BLK_DEV
    indices = jnp.arange(devices_all, dtype=jnp.int32)
    fastest = jnp.max(lax.map(lambda device: jnp.max(signal(pencil_of(prim, device))), indices))
    time_step = COURANT / fastest

    def update(device):
        middle = pencil_of(prim, device)
        under_rows = pencil_of(prim, (device - 1) % devices_all)[:, :, edge_len - 2:]
        over_rows = pencil_of(prim, (device + 1) % devices_all)[:, :, :2]
        y_padded = jnp.concatenate([under_rows, middle, over_rows], 2)
        before_x = pencil_of(prim, (device - GY) % devices_all)[:, edge_len - 2:]
        after_x = pencil_of(prim, (device + GY) % devices_all)[:, :2]
        x_padded = jnp.concatenate([before_x, middle, after_x], 1)
        z_padded = jnp.concatenate([middle[..., -2:], middle, middle[..., :2]], 3)
        result = advance(x_padded, y_padded, z_padded, time_step)
        result = result.reshape(8, edge_len, edge_len, BLK_DEV, edge_len).transpose(0, 3, 1, 2, 4)
        return result.reshape(8, BLK_DEV, edge_len ** 3)
    updated = lax.map(update, indices)
    updated = updated.transpose(1, 0, 2, 3).reshape(8, prim.shape[1], edge_len ** 3)
    target = new_owner * CAP + new_slot
    placed = jnp.zeros((8, devices_all * CAP, edge_len ** 3), jnp.float32).at[:, target].set(updated)
    return placed
```

```python
import functools

import jax
import jax.numpy as jnp
from jax import lax
from jax.experimental import pallas as pl
from jax.experimental.pallas import tpu as pltpu
from jax.sharding import PartitionSpec as P

GY = 16
AXES = ("outer", "inner")
GAMMA = 5.0 / 3.0
COURANT = 0.8
LANES = 128
TILES = 4
FIELDS = 8
BLOCKS = 12
REACH = 6
CAP = 24


def roll(value, shift):
    return pltpu.roll(value, shift % LANES, 1)


def lane_ids(rows):
    return lax.broadcasted_iota(jnp.int32, (rows, LANES), 1)


def half_minmod(former, latter):
    return 0.5 * (
        jnp.maximum(jnp.minimum(former, latter), 0.0)
        + jnp.minimum(jnp.maximum(former, latter), 0.0)
    )


def sound(density, pressure, field_sq):
    pushed = GAMMA * pressure + field_sq
    return pushed * lax.rsqrt(pushed * density)


def squared(state):
    return state[5] * state[5] + state[6] * state[6] + state[7] * state[7]


def conserved(state, field_sq):
    density, pressure = state[0], state[4]
    momentum = [density * state[1 + k] for k in range(3)]
    kinetic = momentum[0] * state[1] + momentum[1] * state[2] + momentum[2] * state[3]
    energy = pressure * (1.0 / (GAMMA - 1.0)) + 0.5 * (kinetic + field_sq)
    return [density, *momentum, energy, state[5], state[6], state[7]]


def flux_parts(state, normal):
    field_sq = squared(state)
    total_pressure = state[4] + 0.5 * field_sq
    whole = conserved(state, field_sq)
    speed, field = state[1 + normal], state[5 + normal]
    along = state[1] * state[5] + state[2] * state[6] + state[3] * state[7]
    momentum = [whole[1 + k] * speed - state[5 + k] * field for k in range(3)]
    momentum[normal] = momentum[normal] + total_pressure
    induction = [
        None if k == normal else state[5 + k] * speed - state[1 + k] * field for k in range(3)
    ]
    energy = (whole[4] + total_pressure) * speed - field * along
    signal = jnp.abs(speed) + sound(state[0], state[4], field_sq)
    return [whole[1 + normal], *momentum, energy, *induction], signal, whole


def twice_face_flux(left, right, normal):
    flux_left, signal_left, whole_left = flux_parts(left, normal)
    flux_right, signal_right, whole_right = flux_parts(right, normal)
    fastest = jnp.maximum(signal_left, signal_right)
    result = []
    for k in range(FIELDS):
        spread = fastest * (whole_right[k] - whole_left[k])
        result.append(-spread if flux_left[k] is None else flux_left[k] + flux_right[k] - spread)
    return result


def cell_rows(tile, k, first=0, count=BLOCKS):
    return pl.ds((first * TILES + tile) * FIELDS + k, count, stride=TILES * FIELDS)


def device_index():
    return lax.axis_index(AXES[0]) * lax.axis_size(AXES[1]) + lax.axis_index(AXES[1])


def prepare_kernel(prim_ref, x_first_ref, x_second_ref, y_inner_ref, y_outer_ref, fastest_ref):
    device = device_index()
    odd_row = (device // GY) % 2 == 1
    odd = device % 2 == 1
    slot = (lane_ids(FIELDS) // 16) % TILES
    for block in range(BLOCKS):
        parts = [
            prim_ref[(block * TILES + tile) * FIELDS : (block * TILES + tile + 1) * FIELDS]
            for tile in range(TILES)
        ]
        low, high = parts[0], roll(parts[0], -48)
        for tile in range(1, TILES):
            low = jnp.where(slot == tile, roll(parts[tile], 16 * tile), low)
            high = jnp.where(slot == tile, roll(parts[tile], 16 * tile - 48), high)
        here = slice(block * FIELDS, (block + 1) * FIELDS)
        x_first_ref[here] = jnp.where(odd_row, parts[0], parts[-1])
        x_second_ref[here] = jnp.where(odd_row, parts[-1], parts[0])
        y_inner_ref[here] = jnp.where(odd, low, high)
        y_outer_ref[here] = jnp.where(odd, high, low)
    best = None
    for tile in range(TILES):
        state = [prim_ref[cell_rows(tile, k)] for k in range(FIELDS)]
        speed = (
            jnp.abs(state[1])
            + jnp.abs(state[2])
            + jnp.abs(state[3])
            + 3.0 * sound(state[0], state[4], squared(state))
        )
        best = speed if best is None else jnp.maximum(best, speed)
    fastest_ref[...] = jnp.broadcast_to(jnp.max(best, keepdims=True), fastest_ref.shape)


def change_kernel(
    prim_ref, x_first_ref, x_second_ref, y_inner_ref, y_outer_ref, own_ref, inner_ref, outer_ref
):
    device = device_index()
    odd_row = (device // GY) % 2 == 1
    odd = device % 2 == 1
    lane = lane_ids(BLOCKS)
    first_half = lane < 64
    y_low = (lane % 64) < 8
    y_high = (lane % 64) >= 56
    z_low = (lane % 8) == 0
    z_high = (lane % 8) == 7
    packed_slot = (lane // 16) % TILES

    def either(first, second, k, flag):
        rows = pl.ds(k, BLOCKS, stride=FIELDS)
        return jnp.where(flag, first[rows], second[rows])

    fields = range(FIELDS)
    cells = [[prim_ref[cell_rows(tile, k)] for k in fields] for tile in range(TILES)]
    total = [[None] * FIELDS for _ in range(TILES)]

    before = [either(x_first_ref, x_second_ref, k, odd_row) for k in fields]
    after = [either(x_second_ref, x_first_ref, k, odd_row) for k in fields]
    line = [before] + cells + [after]
    turned = [[roll(value, 64) for value in part] for part in line]
    lefts, rights = [], []
    for tile in range(TILES + 2):
        left, right = [], []
        for k in fields:
            here = line[tile][k]
            down = turned[max(tile - 1, 0)][k]
            up = turned[min(tile + 1, TILES + 1)][k]
            same = turned[tile][k]
            half = half_minmod(
                here - jnp.where(first_half, down, same), jnp.where(first_half, same, up) - here
            )
            left.append(here + half)
            right.append(roll(here - half, 64))
        lefts.append(left)
        rights.append(right)
    previous = None
    for tile in range(TILES + 1):
        right = [jnp.where(first_half, rights[tile][k], rights[tile + 1][k]) for k in fields]
        face = twice_face_flux(lefts[tile], right, 0)
        turned_face = [roll(value, 64) for value in face]
        if tile > 0:
            for k in fields:
                total[tile - 1][k] = face[k] - jnp.where(
                    first_half, previous[k], turned_face[k]
                )
        previous = turned_face

    low_halo = [either(y_inner_ref, y_outer_ref, k, odd) for k in fields]
    high_halo = [either(y_outer_ref, y_inner_ref, k, odd) for k in fields]
    low_left, low_right, high_right = [], [], []
    for k in fields:
        low, high = cells[0][k], roll(cells[0][k], -48)
        for tile in range(1, TILES):
            low = jnp.where(packed_slot == tile, roll(cells[tile][k], 16 * tile), low)
            high = jnp.where(packed_slot == tile, roll(cells[tile][k], 16 * tile - 48), high)
        outside, edge = low_halo[k], roll(low, 8)
        step = edge - outside
        low_left.append(outside + half_minmod(outside - roll(outside, 8), step))
        low_right.append(edge - half_minmod(step, low - edge))
        outside = high_halo[k]
        high_right.append(
            outside - half_minmod(outside - roll(high, -8), roll(outside, -8) - outside)
        )
    low_face = twice_face_flux(low_left, low_right, 1)
    for tile in range(TILES):
        to_low, to_high = -8 * (2 * tile + 1), 8 * (7 - 2 * tile)
        left, right = [], []
        for k in fields:
            here = cells[tile][k]
            down = jnp.where(y_low, roll(low_halo[k], to_low), roll(here, 8))
            up = jnp.where(y_high, roll(high_halo[k], to_high), roll(here, -8))
            half = half_minmod(here - down, up - here)
            left.append(here + half)
            right.append(
                jnp.where(y_high, roll(high_right[k], to_high), roll(here - half, -8))
            )
        face = twice_face_flux(left, right, 1)
        for k in fields:
            down = jnp.where(y_low, roll(low_face[k], to_low), roll(face[k], 8))
            total[tile][k] = total[tile][k] + (face[k] - down)

    def next_cell(value):
        turned = roll(value, 7)
        turned = jnp.concatenate([turned[1:], turned[:1]], 0)
        return jnp.where(z_high, turned, roll(value, -1))

    def last_cell(value):
        turned = roll(value, -7)
        turned = jnp.concatenate([turned[-1:], turned[:-1]], 0)
        return jnp.where(z_low, turned, roll(value, 1))

    for tile in range(TILES):
        left, right = [], []
        for k in fields:
            here = cells[tile][k]
            half = half_minmod(here - last_cell(here), next_cell(here) - here)
            left.append(here + half)
            right.append(next_cell(here - half))
        face = twice_face_flux(left, right, 2)
        whole = conserved(cells[tile], squared(cells[tile]))
        for k in fields:
            change = total[tile][k] + (face[k] - last_cell(face[k]))
            own_ref.at[0][cell_rows(tile, k)] = whole[k]
            own_ref.at[1][cell_rows(tile, k)] = change

    half = REACH * TILES * FIELDS
    to_inner = pl.multiple_of(jnp.where(odd, 0, half), FIELDS)
    to_outer = pl.multiple_of(jnp.where(odd, half, 0), FIELDS)
    for part in range(2):
        inner_ref[part] = own_ref[part, pl.ds(to_inner, half)]
        outer_ref[part] = own_ref[part, pl.ds(to_outer, half)]


def place_kernel(fastest_ref, own_ref, inner_ref, outer_ref, owner_ref, out_ref, held_ref):
    device = device_index()
    odd = device % 2 == 1
    scale = (0.5 * COURANT) / jnp.max(fastest_ref[...])
    half = REACH * TILES * FIELDS

    def stepped(ref):
        return ref[0] - scale * ref[1]

    inner, outer = stepped(inner_ref), stepped(outer_ref)
    held_ref[:half] = jnp.where(odd, inner, outer)
    held_ref[half : 3 * half] = stepped(own_ref)
    held_ref[3 * half : 4 * half] = jnp.where(odd, outer, inner)
    owners = owner_ref[...]
    first = jnp.sum((owners < device).astype(jnp.int32)) - (device * BLOCKS - REACH)
    count = jnp.sum((owners == device).astype(jnp.int32))
    first = jnp.clip(first, 0, BLOCKS)
    live = lax.broadcasted_iota(jnp.int32, (CAP, LANES), 0) < count
    for k in range(FIELDS):
        for tile in range(TILES):
            value = held_ref[cell_rows(tile, k, first, CAP)]
            out_ref[k, :, tile * LANES : (tile + 1) * LANES] = jnp.where(live, value, 0.0)


def call(kernel, outs, name, flops, scratch=()):
    return pl.pallas_call(
        kernel,
        out_shape=[jax.ShapeDtypeStruct(shape, jnp.float32) for shape in outs],
        scratch_shapes=list(scratch),
        cost_estimate=pl.CostEstimate(flops=flops, bytes_accessed=flops // 8, transcendentals=0),
        name=name,
    )


def swap(value, partner, devices):
    pairs = [(i, partner(i) % devices) for i in range(devices) if partner(i) is not None]
    return lax.ppermute(value, AXES, pairs)


def per_device(ranks, prim, new_owner, new_slot):
    del new_slot
    devices = lax.axis_size(AXES)
    rows = BLOCKS * TILES * FIELDS
    raw = prim.reshape(FIELDS, BLOCKS, TILES, LANES).transpose(1, 2, 0, 3).reshape(rows, LANES)
    side = (BLOCKS * FIELDS, LANES)
    x_first, x_second, y_inner, y_outer, fastest = call(
        prepare_kernel, [side, side, side, side, (devices, LANES)], "prepare", 10**6
    )(raw)
    everyone = lax.all_to_all(fastest, AXES, 0, 0, tiled=True)

    def within(i, j):
        return j if 0 <= j < devices and i // ranks == j // ranks else None

    x_first = swap(x_first, lambda i: i + GY if (i // GY) % 2 == 0 else i - GY, devices)
    x_second = swap(x_second, lambda i: i + GY if (i // GY) % 2 == 1 else i - GY, devices)
    y_outer = swap(y_outer, lambda i: i + 1 if i % 2 == 1 else i - 1, devices)
    y_inner = swap(y_inner, lambda i: i ^ 1, devices)
    half = (2, rows // 2, LANES)
    own, to_inner, to_outer = call(
        change_kernel, [(2, rows, LANES), half, half], "change", 2 * 10**7
    )(raw, x_first, x_second, y_inner, y_outer)
    from_outer = swap(to_outer, lambda i: within(i, i + 1 if i % 2 == 1 else i - 1), devices)
    from_inner = swap(to_inner, lambda i: i ^ 1, devices)
    (placed,) = call(
        place_kernel,
        [(FIELDS, CAP, TILES * LANES)],
        "place",
        10**6,
        [pltpu.VMEM((3 * rows, LANES), jnp.float32)],
    )(everyone, own, from_inner, from_outer, new_owner.reshape(-1, LANES))
    return placed


def solution(mesh):
    return jax.shard_map(
        functools.partial(per_device, mesh.shape["inner"]),
        mesh=mesh,
        in_specs=(P(None, AXES, None), P(), P()),
        out_specs=P(None, AXES, None),
        check_vma=False,
    )
```

```python
import functools

import jax
import jax.numpy as jnp
from jax import lax
from jax.experimental import pallas as pl
from jax.experimental.pallas import tpu as pltpu
from jax.sharding import PartitionSpec as P


GY = 16
AXES = ("outer", "inner")
GAMMA = 5.0 / 3.0
COURANT = 0.8
LANES = 128
TILES = 4
FIELDS = 8
BLOCKS = 12
REACH = 6
CAP = 24


def roll(value, shift):
    return pltpu.roll(value, shift % LANES, 1)


def lane_ids(rows):
    return lax.broadcasted_iota(jnp.int32, (rows, LANES), 1)


def half_minmod(former, latter):
    return 0.5 * (
        jnp.maximum(jnp.minimum(former, latter), 0.0)
        + jnp.minimum(jnp.maximum(former, latter), 0.0)
    )


def sound(density, pressure, field_sq):
    pushed = GAMMA * pressure + field_sq
    return pushed * lax.rsqrt(pushed * density)


def squared(state):
    return state[5] * state[5] + state[6] * state[6] + state[7] * state[7]


def conserved(state, field_sq):
    density, pressure = state[0], state[4]
    momentum = [density * state[1 + k] for k in range(3)]
    kinetic = momentum[0] * state[1] + momentum[1] * state[2] + momentum[2] * state[3]
    energy = pressure * (1.0 / (GAMMA - 1.0)) + 0.5 * (kinetic + field_sq)
    return [density, *momentum, energy, state[5], state[6], state[7]]


def flux_parts(state, normal):
    field_sq = squared(state)
    total_pressure = state[4] + 0.5 * field_sq
    whole = conserved(state, field_sq)
    speed, field = state[1 + normal], state[5 + normal]
    along = state[1] * state[5] + state[2] * state[6] + state[3] * state[7]
    momentum = [whole[1 + k] * speed - state[5 + k] * field for k in range(3)]
    momentum[normal] = momentum[normal] + total_pressure
    induction = [
        None if k == normal else state[5 + k] * speed - state[1 + k] * field for k in range(3)
    ]
    energy = (whole[4] + total_pressure) * speed - field * along
    signal = jnp.abs(speed) + sound(state[0], state[4], field_sq)
    return [whole[1 + normal], *momentum, energy, *induction], signal, whole


def twice_face_flux(left, right, normal):
    flux_left, signal_left, whole_left = flux_parts(left, normal)
    flux_right, signal_right, whole_right = flux_parts(right, normal)
    fastest = jnp.maximum(signal_left, signal_right)
    result = []
    for k in range(FIELDS):
        spread = fastest * (whole_right[k] - whole_left[k])
        result.append(-spread if flux_left[k] is None else flux_left[k] + flux_right[k] - spread)
    return result


def cell_rows(tile, k, first=0, count=BLOCKS):
    return pl.ds((first * TILES + tile) * FIELDS + k, count, stride=TILES * FIELDS)


def device_index():
    return lax.axis_index(AXES[0]) * lax.axis_size(AXES[1]) + lax.axis_index(AXES[1])


def prepare_kernel(prim_ref, x_first_ref, x_second_ref, y_inner_ref, y_outer_ref, fastest_ref):
    device = device_index()
    odd_row = (device // GY) % 2 == 1
    odd = device % 2 == 1
    slot = (lane_ids(FIELDS) // 16) % TILES
    for block in range(BLOCKS):
        parts = [
            prim_ref[(block * TILES + tile) * FIELDS : (block * TILES + tile + 1) * FIELDS]
            for tile in range(TILES)
        ]
        low, high = parts[0], roll(parts[0], -48)
        for tile in range(1, TILES):
            low = jnp.where(slot == tile, roll(parts[tile], 16 * tile), low)
            high = jnp.where(slot == tile, roll(parts[tile], 16 * tile - 48), high)
        here = slice(block * FIELDS, (block + 1) * FIELDS)
        x_first_ref[here] = jnp.where(odd_row, parts[0], parts[-1])
        x_second_ref[here] = jnp.where(odd_row, parts[-1], parts[0])
        y_inner_ref[here] = jnp.where(odd, low, high)
        y_outer_ref[here] = jnp.where(odd, high, low)
    best = None
    for tile in range(TILES):
        state = [prim_ref[cell_rows(tile, k)] for k in range(FIELDS)]
        speed = (
            jnp.abs(state[1])
            + jnp.abs(state[2])
            + jnp.abs(state[3])
            + 3.0 * sound(state[0], state[4], squared(state))
        )
        best = speed if best is None else jnp.maximum(best, speed)
    fastest_ref[...] = jnp.broadcast_to(jnp.max(best, keepdims=True), fastest_ref.shape)


def change_kernel(
    prim_ref, x_first_ref, x_second_ref, y_inner_ref, y_outer_ref, own_ref, inner_ref, outer_ref
):
    device = device_index()
    odd_row = (device // GY) % 2 == 1
    odd = device % 2 == 1
    lane = lane_ids(BLOCKS)
    first_half = lane < 64
    y_low = (lane % 64) < 8
    y_high = (lane % 64) >= 56
    z_low = (lane % 8) == 0
    z_high = (lane % 8) == 7
    packed_slot = (lane // 16) % TILES

    def either(first, second, k, flag):
        rows = pl.ds(k, BLOCKS, stride=FIELDS)
        return jnp.where(flag, first[rows], second[rows])

    fields = range(FIELDS)
    cells = [[prim_ref[cell_rows(tile, k)] for k in fields] for tile in range(TILES)]
    total = [[None] * FIELDS for _ in range(TILES)]

    before = [either(x_first_ref, x_second_ref, k, odd_row) for k in fields]
    after = [either(x_second_ref, x_first_ref, k, odd_row) for k in fields]
    line = [before] + cells + [after]
    turned = [[roll(value, 64) for value in part] for part in line]
    lefts, rights = [], []
    for tile in range(TILES + 2):
        left, right = [], []
        for k in fields:
            here = line[tile][k]
            down = turned[max(tile - 1, 0)][k]
            up = turned[min(tile + 1, TILES + 1)][k]
            same = turned[tile][k]
            half = half_minmod(
                here - jnp.where(first_half, down, same), jnp.where(first_half, same, up) - here
            )
            left.append(here + half)
            right.append(roll(here - half, 64))
        lefts.append(left)
        rights.append(right)
    previous = None
    for tile in range(TILES + 1):
        right = [jnp.where(first_half, rights[tile][k], rights[tile + 1][k]) for k in fields]
        face = twice_face_flux(lefts[tile], right, 0)
        turned_face = [roll(value, 64) for value in face]
        if tile > 0:
            for k in fields:
                total[tile - 1][k] = face[k] - jnp.where(
                    first_half, previous[k], turned_face[k]
                )
        previous = turned_face

    low_halo = [either(y_inner_ref, y_outer_ref, k, odd) for k in fields]
    high_halo = [either(y_outer_ref, y_inner_ref, k, odd) for k in fields]
    low_left, low_right, high_right = [], [], []
    for k in fields:
        low, high = cells[0][k], roll(cells[0][k], -48)
        for tile in range(1, TILES):
            low = jnp.where(packed_slot == tile, roll(cells[tile][k], 16 * tile), low)
            high = jnp.where(packed_slot == tile, roll(cells[tile][k], 16 * tile - 48), high)
        outside, edge = low_halo[k], roll(low, 8)
        step = edge - outside
        low_left.append(outside + half_minmod(outside - roll(outside, 8), step))
        low_right.append(edge - half_minmod(step, low - edge))
        outside = high_halo[k]
        high_right.append(
            outside - half_minmod(outside - roll(high, -8), roll(outside, -8) - outside)
        )
    low_face = twice_face_flux(low_left, low_right, 1)
    for tile in range(TILES):
        to_low, to_high = -8 * (2 * tile + 1), 8 * (7 - 2 * tile)
        left, right = [], []
        for k in fields:
            here = cells[tile][k]
            down = jnp.where(y_low, roll(low_halo[k], to_low), roll(here, 8))
            up = jnp.where(y_high, roll(high_halo[k], to_high), roll(here, -8))
            half = half_minmod(here - down, up - here)
            left.append(here + half)
            right.append(
                jnp.where(y_high, roll(high_right[k], to_high), roll(here - half, -8))
            )
        face = twice_face_flux(left, right, 1)
        for k in fields:
            down = jnp.where(y_low, roll(low_face[k], to_low), roll(face[k], 8))
            total[tile][k] = total[tile][k] + (face[k] - down)

    def next_cell(value):
        turned = roll(value, 7)
        turned = jnp.concatenate([turned[1:], turned[:1]], 0)
        return jnp.where(z_high, turned, roll(value, -1))

    def last_cell(value):
        turned = roll(value, -7)
        turned = jnp.concatenate([turned[-1:], turned[:-1]], 0)
        return jnp.where(z_low, turned, roll(value, 1))

    for tile in range(TILES):
        left, right = [], []
        for k in fields:
            here = cells[tile][k]
            half = half_minmod(here - last_cell(here), next_cell(here) - here)
            left.append(here + half)
            right.append(next_cell(here - half))
        face = twice_face_flux(left, right, 2)
        whole = conserved(cells[tile], squared(cells[tile]))
        for k in fields:
            change = total[tile][k] + (face[k] - last_cell(face[k]))
            own_ref.at[0][cell_rows(tile, k)] = whole[k]
            own_ref.at[1][cell_rows(tile, k)] = change

    half = REACH * TILES * FIELDS
    to_inner = pl.multiple_of(jnp.where(odd, 0, half), FIELDS)
    to_outer = pl.multiple_of(jnp.where(odd, half, 0), FIELDS)
    for part in range(2):
        inner_ref[part] = own_ref[part, pl.ds(to_inner, half)]
        outer_ref[part] = own_ref[part, pl.ds(to_outer, half)]


def place_kernel(fastest_ref, own_ref, inner_ref, outer_ref, owner_ref, out_ref, held_ref):
    device = device_index()
    odd = device % 2 == 1
    scale = (0.5 * COURANT) / jnp.max(fastest_ref[...])
    half = REACH * TILES * FIELDS

    def stepped(ref):
        return ref[0] - scale * ref[1]

    inner, outer = stepped(inner_ref), stepped(outer_ref)
    held_ref[:half] = jnp.where(odd, inner, outer)
    held_ref[half : 3 * half] = stepped(own_ref)
    held_ref[3 * half : 4 * half] = jnp.where(odd, outer, inner)
    owners = owner_ref[...]
    first = jnp.sum((owners < device).astype(jnp.int32)) - (device * BLOCKS - REACH)
    count = jnp.sum((owners == device).astype(jnp.int32))
    first = jnp.clip(first, 0, BLOCKS)
    live = lax.broadcasted_iota(jnp.int32, (CAP, LANES), 0) < count
    for k in range(FIELDS):
        for tile in range(TILES):
            value = held_ref[cell_rows(tile, k, first, CAP)]
            out_ref[k, :, tile * LANES : (tile + 1) * LANES] = jnp.where(live, value, 0.0)


def call(kernel, outs, flops, scratch=()):
    return pl.pallas_call(
        kernel,
        out_shape=[jax.ShapeDtypeStruct(shape, jnp.float32) for shape in outs],
        scratch_shapes=list(scratch),
        cost_estimate=pl.CostEstimate(flops=flops, bytes_accessed=flops // 8, transcendentals=0),
        compiler_params=pltpu.CompilerParams(vmem_limit_bytes=8 * 2**20),
    )


def swap(value, partner, devices):
    pairs = [(i, partner(i) % devices) for i in range(devices) if partner(i) is not None]
    return lax.ppermute(value, AXES, pairs)


def per_device(ranks, prim, new_owner, new_slot):
    del new_slot
    devices = lax.axis_size(AXES)
    rows = BLOCKS * TILES * FIELDS
    raw = prim.reshape(FIELDS, BLOCKS, TILES, LANES).transpose(1, 2, 0, 3).reshape(rows, LANES)
    side = (BLOCKS * FIELDS, LANES)
    x_first, x_second, y_inner, y_outer, fastest = call(
        prepare_kernel, [side, side, side, side, (devices, LANES)], 10**6
    )(raw)
    everyone = lax.all_to_all(fastest, AXES, 0, 0, tiled=True)

    def within(i, j):
        return j if 0 <= j < devices and i // ranks == j // ranks else None

    x_first = swap(x_first, lambda i: i + GY if (i // GY) % 2 == 0 else i - GY, devices)
    x_second = swap(x_second, lambda i: i + GY if (i // GY) % 2 == 1 else i - GY, devices)
    y_outer = swap(y_outer, lambda i: i + 1 if i % 2 == 1 else i - 1, devices)
    y_inner = swap(y_inner, lambda i: i ^ 1, devices)
    half = (2, rows // 2, LANES)
    own, to_inner, to_outer = call(
        change_kernel, [(2, rows, LANES), half, half], 2 * 10**7
    )(raw, x_first, x_second, y_inner, y_outer)
    from_outer = swap(to_outer, lambda i: within(i, i + 1 if i % 2 == 1 else i - 1), devices)
    from_inner = swap(to_inner, lambda i: i ^ 1, devices)
    (placed,) = call(
        place_kernel,
        [(FIELDS, CAP, TILES * LANES)],
        10**6,
        [pltpu.VMEM((3 * rows, LANES), jnp.float32)],
    )(everyone, own, from_inner, from_outer, new_owner.reshape(-1, LANES))
    return placed


def solution(mesh):
    return jax.shard_map(
        functools.partial(per_device, mesh.shape["inner"]),
        mesh=mesh,
        in_specs=(P(None, AXES, None), P(), P()),
        out_specs=P(None, AXES, None),
        check_vma=False,
    )
```

```python
import functools

import jax
import jax.numpy as jnp
from jax import lax
from jax.experimental import pallas as pl
from jax.experimental.pallas import tpu as pltpu
from jax.sharding import PartitionSpec as P


BE = 8
GY = 16
AXES = ("outer", "inner")
GAMMA = 5.0 / 3.0
COURANT = 0.8
LANES = 128
TILES = 4
FIELDS = 8
BLOCKS = 12
REACH = 6
CAP = 24
ROWS = 16
HELD = 40
SIDE = FIELDS * 2 * BE
PITCH = BE + 2


def roll(value, shift):
    return pltpu.roll(value, shift % LANES, 1)


def half_minmod(former, latter):
    return 0.5 * (
        jnp.maximum(jnp.minimum(former, latter), 0.0)
        + jnp.minimum(jnp.maximum(former, latter), 0.0)
    )


def sound(density, pressure, field_sq):
    pushed = GAMMA * pressure + field_sq
    return pushed * lax.rsqrt(pushed * density)


def squared(state):
    return state[5] * state[5] + state[6] * state[6] + state[7] * state[7]


def conserved(state, field_sq):
    density, pressure = state[0], state[4]
    momentum = [density * state[1 + k] for k in range(3)]
    kinetic = momentum[0] * state[1] + momentum[1] * state[2] + momentum[2] * state[3]
    energy = pressure * (1.0 / (GAMMA - 1.0)) + 0.5 * (kinetic + field_sq)
    return [density, *momentum, energy, state[5], state[6], state[7]]


def flux_parts(state, normal):
    field_sq = squared(state)
    total_pressure = state[4] + 0.5 * field_sq
    whole = conserved(state, field_sq)
    speed, field = state[1 + normal], state[5 + normal]
    along = state[1] * state[5] + state[2] * state[6] + state[3] * state[7]
    momentum = [whole[1 + k] * speed - state[5 + k] * field for k in range(3)]
    momentum[normal] = momentum[normal] + total_pressure
    induction = [
        None if k == normal else state[5 + k] * speed - state[1 + k] * field for k in range(3)
    ]
    energy = (whole[4] + total_pressure) * speed - field * along
    signal = jnp.abs(speed) + sound(state[0], state[4], field_sq)
    return [whole[1 + normal], *momentum, energy, *induction], signal, whole


def twice_face_flux(left, right, normal):
    flux_left, signal_left, whole_left = flux_parts(left, normal)
    flux_right, signal_right, whole_right = flux_parts(right, normal)
    fastest = jnp.maximum(signal_left, signal_right)
    result = []
    for k in range(FIELDS):
        spread = fastest * (whole_right[k] - whole_left[k])
        result.append(-spread if flux_left[k] is None else flux_left[k] + flux_right[k] - spread)
    return result


def rows_of(index):
    return slice(index * ROWS, (index + 1) * ROWS)


def device_index():
    return lax.axis_index(AXES[0]) * lax.axis_size(AXES[1]) + lax.axis_index(AXES[1])


def turn(first, second):
    row = lax.broadcasted_iota(jnp.int32, (8, LANES), 0)
    lane = lax.broadcasted_iota(jnp.int32, (8, LANES), 1)
    group, place = lane // 8, lane % 8

    def along(value, source):
        return jnp.take_along_axis(value, source, axis=1, mode="promise_in_bounds")

    def across(index):
        source = (group - row - index) % 16
        picked = [
            jnp.take_along_axis(value, source % 8, axis=0, mode="promise_in_bounds")
            for value in (first, second)
        ]
        return jnp.where(source < 8, picked[0], picked[1])

    first = along(first, (group - row) % 16 * 8 + place)
    second = along(second, (group - row - 8) % 16 * 8 + place)
    upper, lower = across(0), across(8)
    return (
        along(upper, (group + row) % 16 * 8 + place),
        along(lower, (group + row + 8) % 16 * 8 + place),
    )


def prepare_kernel(
    prim_ref, x_first_ref, x_second_ref, y_inner_ref, y_outer_ref, fastest_ref, cells_ref, whole_ref
):
    device = device_index()
    odd_row = (device // GY) % 2 == 1
    odd = device % 2 == 1
    cells = []
    for k in range(FIELDS):
        line = []
        for tile in range(TILES):
            part = prim_ref[pl.ds(tile * FIELDS + k, BLOCKS, stride=TILES * FIELDS)]
            line.append(jnp.concatenate([part, part[:1], part[:2], part[-1:]], 0))
        cells.append(line)
    best = None
    for tile in range(TILES):
        state = [cells[k][tile] for k in range(FIELDS)]
        field_sq = squared(state)
        speed = (
            jnp.abs(state[1])
            + jnp.abs(state[2])
            + jnp.abs(state[3])
            + 3.0 * sound(state[0], state[4], field_sq)
        )
        best = speed if best is None else jnp.maximum(best, speed)
        for k, value in enumerate(conserved(state, field_sq)):
            whole_ref[rows_of(k * TILES + tile)] = value
    fastest_ref[...] = jnp.broadcast_to(jnp.max(best, keepdims=True), fastest_ref.shape)
    for k in range(FIELDS):
        for tile in range(TILES):
            halves = turn(cells[k][tile][:8], cells[k][tile][8:])
            base = (k * BE + 2 * tile) * BE
            cells_ref[base : base + 8], cells_ref[base + 8 : base + 16] = halves
    to_first = jnp.where(odd_row, 0, BE - 2)
    to_second = jnp.where(odd_row, BE - 2, 0)
    to_inner = jnp.where(odd, 0, BE - 2)
    to_outer = jnp.where(odd, BE - 2, 0)
    for k in range(FIELDS):
        base, there = k * BE * BE, slice(k * 2 * BE, (k + 1) * 2 * BE)
        for start, ref in ((to_first, x_first_ref), (to_second, x_second_ref)):
            ref[there] = cells_ref[pl.ds(pl.multiple_of(base + start * BE, BE), 2 * BE)]
        for start, ref in ((to_inner, y_inner_ref), (to_outer, y_outer_ref)):
            for layer in range(2):
                row = (2 * k + layer) * BE
                ref[row : row + BE] = cells_ref[pl.ds(base + start + layer, BE, stride=BE)]
    send_half(whole_ref, y_inner_ref, y_outer_ref, SIDE, odd)


def send_half(source, inner_ref, outer_ref, base, odd):
    to_inner = jnp.where(odd, 0, REACH)
    to_outer = jnp.where(odd, REACH, 0)
    for row in range(FIELDS * TILES):
        there = slice(base + row * REACH, base + (row + 1) * REACH)
        inner_ref[there] = source[pl.ds(row * ROWS + to_inner, REACH)]
        outer_ref[there] = source[pl.ds(row * ROWS + to_outer, REACH)]


def change_kernel(
    cells_ref,
    x_first_ref,
    x_second_ref,
    y_inner_ref,
    y_outer_ref,
    own_ref,
    inner_ref,
    outer_ref,
    line_ref,
    right_ref,
    face_ref,
):
    device = device_index()
    odd_row = (device // GY) % 2 == 1
    odd = device % 2 == 1
    fields = range(FIELDS)

    def cell(x, k):
        return cells_ref[(k * BE + x) * BE : (k * BE + x + 1) * BE]

    def halo(first, second, k, layer, flag):
        rows = slice((2 * k + layer) * BE, (2 * k + layer + 1) * BE)
        return jnp.where(flag, first[rows], second[rows])

    def padded(x, k, y):
        return slice((k * BE + x) * PITCH + y + 1, (k * BE + x) * PITCH + y + 1 + BE)

    def all_x(k, y):
        return pl.ds(k * BE * PITCH + y + 1, BE, stride=PITCH)

    def column(x):
        if x < 0:
            return [halo(x_first_ref, x_second_ref, k, x + 2, odd_row) for k in fields]
        if x >= BE:
            return [halo(x_second_ref, x_first_ref, k, x - BE, odd_row) for k in fields]
        return [cell(x, k) for k in fields]

    total = [None] * BE
    here, up = column(-2), column(-1)
    ahead = [up[k] - here[k] for k in fields]
    left = last_face = None
    for x in range(-1, BE + 1):
        here, up, behind = up, column(x + 1), ahead
        ahead = [up[k] - here[k] for k in fields]
        half = [half_minmod(behind[k], ahead[k]) for k in fields]
        if left is not None:
            face = twice_face_flux(left, [here[k] - half[k] for k in fields], 0)
            if last_face is not None:
                total[x - 1] = [face[k] - last_face[k] for k in fields]
            last_face = face
        left = [here[k] + half[k] for k in fields]

    low_left, low_right = [], []
    for k in fields:
        far = halo(y_inner_ref, y_outer_ref, k, 0, odd)
        near = halo(y_inner_ref, y_outer_ref, k, 1, odd)
        edge = cells_ref[pl.ds(k * BE * BE, BE, stride=BE)]
        after = cells_ref[pl.ds(k * BE * BE + 1, BE, stride=BE)]
        low_left.append(near + half_minmod(near - far, edge - near))
        low_right.append(edge - half_minmod(edge - near, after - edge))
        line_ref[all_x(k, -1)] = near
        near = halo(y_outer_ref, y_inner_ref, k, 0, odd)
        far = halo(y_outer_ref, y_inner_ref, k, 1, odd)
        edge = cells_ref[pl.ds(k * BE * BE + BE - 1, BE, stride=BE)]
        line_ref[all_x(k, BE)] = near
        right_ref[all_x(k, BE)] = near - half_minmod(near - edge, far - near)
    for k, value in enumerate(twice_face_flux(low_left, low_right, 1)):
        face_ref[all_x(k, -1)] = value
    for x in range(BE):
        for k in fields:
            line_ref[padded(x, k, 0)] = cell(x, k)
    for x in range(BE):
        state = [cell(x, k) for k in fields]
        left = []
        for k in fields:
            half = half_minmod(
                state[k] - line_ref[padded(x, k, -1)], line_ref[padded(x, k, 1)] - state[k]
            )
            left.append(state[k] + half)
            right_ref[padded(x, k, 0)] = state[k] - half
        face = twice_face_flux(left, [right_ref[padded(x, k, 1)] for k in fields], 1)
        for k in fields:
            face_ref[padded(x, k, 0)] = face[k]
        for k in fields:
            total[x][k] = total[x][k] + (face[k] - face_ref[padded(x, k, -1)])

        left, right = [], []
        for k in fields:
            ahead = roll(state[k], -1) - state[k]
            half = half_minmod(roll(ahead, 1), ahead)
            left.append(state[k] + half)
            right.append(roll(state[k] - half, -1))
        face = twice_face_flux(left, right, 2)
        for k in fields:
            total[x][k] = total[x][k] + (face[k] - roll(face[k], 1))

    for k in fields:
        for tile in range(TILES):
            base = (k * TILES + tile) * ROWS
            halves = turn(total[2 * tile][k], total[2 * tile + 1][k])
            own_ref[base : base + 8], own_ref[base + 8 : base + 16] = halves
    send_half(own_ref, inner_ref, outer_ref, 0, odd)


def place_kernel(
    fastest_ref,
    whole_ref,
    change_ref,
    whole_inner_ref,
    whole_outer_ref,
    inner_ref,
    outer_ref,
    owner_ref,
    out_ref,
    held_ref,
):
    device = device_index()
    odd = device % 2 == 1
    owners = owner_ref[...]
    first = jnp.sum((owners < device).astype(jnp.int32)) - (device * BLOCKS - REACH)
    count = jnp.sum((owners == device).astype(jnp.int32))
    first = jnp.clip(first, 0, BLOCKS) + 2
    scale = (0.5 * COURANT) / jnp.max(fastest_ref[...])
    live = lax.broadcasted_iota(jnp.int32, (CAP, LANES), 0) < count
    for row in range(FIELDS * TILES):
        there = slice(row * REACH, (row + 1) * REACH)
        sent = slice(SIDE + row * REACH, SIDE + (row + 1) * REACH)
        inner = whole_inner_ref[sent] - scale * inner_ref[there]
        outer = whole_outer_ref[sent] - scale * outer_ref[there]
        base = row * HELD
        held_ref[base + 8 : base + 8 + ROWS] = (
            whole_ref[rows_of(row)] - scale * change_ref[rows_of(row)]
        )
        held_ref[base + 2 : base + 8] = jnp.where(odd, inner, outer)
        held_ref[base + 20 : base + 26] = jnp.where(odd, outer, inner)
    for row in range(FIELDS * TILES):
        k, tile = divmod(row, TILES)
        value = held_ref[pl.ds(row * HELD + first, CAP)]
        out_ref[k, :, tile * LANES : (tile + 1) * LANES] = jnp.where(live, value, 0.0)


def call(kernel, outs, flops, scratch=()):
    return pl.pallas_call(
        kernel,
        out_shape=[
            jax.ShapeDtypeStruct(out if isinstance(out, tuple) else (out, LANES), jnp.float32)
            for out in outs
        ],
        scratch_shapes=list(scratch),
        cost_estimate=pl.CostEstimate(flops=flops, bytes_accessed=flops // 8, transcendentals=0),
        compiler_params=pltpu.CompilerParams(vmem_limit_bytes=8 * 2**20),
    )


def swap(value, partner, devices):
    pairs = [(i, partner(i) % devices) for i in range(devices) if partner(i) is not None]
    return lax.ppermute(value, AXES, pairs)


def per_device(ranks, prim, new_owner, new_slot):
    del new_slot
    devices = lax.axis_size(AXES)
    raw = prim.reshape(FIELDS, BLOCKS, TILES, LANES).transpose(1, 2, 0, 3).reshape(-1, LANES)
    half = FIELDS * TILES * REACH
    whole = FIELDS * TILES * ROWS
    x_first, x_second, y_inner, y_outer, fastest, cells, conserved_own = call(
        prepare_kernel,
        [SIDE, SIDE, SIDE + half, SIDE + half, devices, FIELDS * BE * BE, whole],
        10**6,
    )(raw)
    everyone = lax.all_to_all(fastest, AXES, 0, 0, tiled=True)

    def within(i, j):
        return j if 0 <= j < devices and i // ranks == j // ranks else None

    x_first = swap(x_first, lambda i: i + GY if (i // GY) % 2 == 0 else i - GY, devices)
    x_second = swap(x_second, lambda i: i + GY if (i // GY) % 2 == 1 else i - GY, devices)
    y_outer = swap(y_outer, lambda i: i + 1 if i % 2 == 1 else i - 1, devices)
    y_inner = swap(y_inner, lambda i: i ^ 1, devices)
    padded = pltpu.VMEM((FIELDS * BE * PITCH, LANES), jnp.float32)
    own, to_inner, to_outer = call(
        change_kernel, [whole, half, half], 2 * 10**7, [padded, padded, padded]
    )(cells, x_first, x_second, y_inner, y_outer)
    from_outer = swap(to_outer, lambda i: within(i, i + 1 if i % 2 == 1 else i - 1), devices)
    from_inner = swap(to_inner, lambda i: i ^ 1, devices)
    (placed,) = call(
        place_kernel,
        [(FIELDS, CAP, TILES * LANES)],
        10**6,
        [pltpu.VMEM((FIELDS * TILES * HELD, LANES), jnp.float32)],
    )(everyone, conserved_own, own, y_inner, y_outer, from_inner, from_outer, new_owner.reshape(-1, LANES))
    return placed


def solution(mesh):
    return jax.shard_map(
        functools.partial(per_device, mesh.shape["inner"]),
        mesh=mesh,
        in_specs=(P(None, AXES, None), P(), P()),
        out_specs=P(None, AXES, None),
        check_vma=False,
    )
```

```python
import functools

import jax
import jax.numpy as jnp
from jax import lax
from jax.experimental import pallas as pl
from jax.experimental.pallas import tpu as pltpu
from jax.sharding import PartitionSpec as P


BE = 8
GY = 16
AXES = ("outer", "inner")
GAMMA = 5.0 / 3.0
COURANT = 0.8
LANES = 128
TILES = 4
FIELDS = 8
BLOCKS = 12
REACH = 6
CAP = 24
ROWS = 16
HELD = 40
SIDE = FIELDS * 2 * BE
PITCH = BE + 2
APART = FIELDS + 1
CHUNKS = 4


def roll(value, shift):
    return pltpu.roll(value, shift % LANES, 1)


def half_minmod(former, latter):
    return 0.5 * (
        jnp.maximum(jnp.minimum(former, latter), 0.0)
        + jnp.minimum(jnp.maximum(former, latter), 0.0)
    )


def sound(density, pressure, field_sq):
    pushed = GAMMA * pressure + field_sq
    return pushed * lax.rsqrt(pushed * density)


def squared(state):
    return state[5] * state[5] + state[6] * state[6] + state[7] * state[7]


def conserved(state, field_sq):
    density, pressure = state[0], state[4]
    momentum = [density * state[1 + k] for k in range(3)]
    kinetic = momentum[0] * state[1] + momentum[1] * state[2] + momentum[2] * state[3]
    energy = pressure * (1.0 / (GAMMA - 1.0)) + 0.5 * (kinetic + field_sq)
    return [density, *momentum, energy, state[5], state[6], state[7]]


def flux_parts(state, normal):
    field_sq = squared(state)
    total_pressure = state[4] + 0.5 * field_sq
    whole = conserved(state, field_sq)
    speed, field = state[1 + normal], state[5 + normal]
    along = state[1] * state[5] + state[2] * state[6] + state[3] * state[7]
    momentum = [whole[1 + k] * speed - state[5 + k] * field for k in range(3)]
    momentum[normal] = momentum[normal] + total_pressure
    induction = [
        None if k == normal else state[5 + k] * speed - state[1 + k] * field for k in range(3)
    ]
    energy = (whole[4] + total_pressure) * speed - field * along
    signal = jnp.abs(speed) + sound(state[0], state[4], field_sq)
    return [whole[1 + normal], *momentum, energy, *induction], signal, whole


def twice_face_flux(left, right, normal):
    flux_left, signal_left, whole_left = flux_parts(left, normal)
    flux_right, signal_right, whole_right = flux_parts(right, normal)
    fastest = jnp.maximum(signal_left, signal_right)
    result = []
    for k in range(FIELDS):
        spread = fastest * (whole_right[k] - whole_left[k])
        result.append(-spread if flux_left[k] is None else flux_left[k] + flux_right[k] - spread)
    return result


def rows_of(index):
    return slice(index * ROWS, (index + 1) * ROWS)


def device_index():
    return lax.axis_index(AXES[0]) * lax.axis_size(AXES[1]) + lax.axis_index(AXES[1])


def turn(first, second):
    row = lax.broadcasted_iota(jnp.int32, (8, LANES), 0)
    group = lax.broadcasted_iota(jnp.int32, (8, LANES), 1) // 8

    def skewed(value, shift):
        return pltpu.roll(value, shift, 1, stride=8, stride_axis=0)

    def across(value, source):
        return jnp.take_along_axis(value, source, axis=0, mode="promise_in_bounds")

    first, second = skewed(first, 0), skewed(second, 64)

    def picked(index):
        source = (row + group + index) & 15
        return jnp.where(source < 8, across(first, source & 7), across(second, source & 7))

    upper, lower = skewed(picked(1), 8), skewed(picked(9), 72)
    return across(lower, 7 - row), across(upper, 7 - row)


def prepare_kernel(
    prim_ref,
    x_first_ref,
    x_second_ref,
    y_inner_ref,
    y_outer_ref,
    fastest_ref,
    cells_ref,
    whole_ref,
    raw_ref,
    spread_ref,
    filled_ref,
    arrived,
    left,
):
    device = device_index()
    odd_row = (device // GY) % 2 == 1
    odd = device % 2 == 1
    part = TILES * FIELDS * BLOCKS // CHUNKS
    copies = [
        pltpu.make_async_copy(
            prim_ref.at[pl.ds(i * part, part)], raw_ref.at[pl.ds(i * part, part)], arrived.at[i]
        )
        for i in range(CHUNKS)
    ]
    for copy in copies:
        copy.start()
    for block in range(BLOCKS):
        if block % (BLOCKS // CHUNKS) == 0:
            copies[block // (BLOCKS // CHUNKS)].wait()
        rows = [block]
        if block == 0:
            rows += [12, 13, 14]
        if block == BLOCKS - 1:
            rows += [15]
        for tile in range(TILES):
            value = raw_ref[(block * TILES + tile) * FIELDS : (block * TILES + tile + 1) * FIELDS]
            for row in rows:
                base = (tile * ROWS + row) * APART
                spread_ref[base : base + FIELDS] = value

    def cell(k, tile, half):
        return spread_ref[pl.ds((tile * ROWS + 8 * half) * APART + k, 8, stride=APART)]

    best = None
    for tile in range(TILES):
        for half in range(2):
            state = [cell(k, tile, half) for k in range(FIELDS)]
            field_sq = squared(state)
            speed = (
                jnp.abs(state[1])
                + jnp.abs(state[2])
                + jnp.abs(state[3])
                + 3.0 * sound(state[0], state[4], field_sq)
            )
            best = speed if best is None else jnp.maximum(best, speed)
            for k, value in enumerate(conserved(state, field_sq)):
                base = (k * TILES + tile) * ROWS + 8 * half
                whole_ref[base : base + 8] = value
    filled_ref[...] = jnp.broadcast_to(jnp.max(best, keepdims=True), filled_ref.shape)
    leaving = pltpu.make_async_copy(filled_ref, fastest_ref, left)
    leaving.start()
    for k in range(FIELDS):
        for tile in range(TILES):
            halves = turn(cell(k, tile, 0), cell(k, tile, 1))
            base = (k * BE + 2 * tile) * BE
            cells_ref[base : base + 8], cells_ref[base + 8 : base + 16] = halves
    to_first = jnp.where(odd_row, 0, BE - 2)
    to_second = jnp.where(odd_row, BE - 2, 0)
    to_inner = jnp.where(odd, 0, BE - 2)
    to_outer = jnp.where(odd, BE - 2, 0)
    for k in range(FIELDS):
        base, there = k * BE * BE, slice(k * 2 * BE, (k + 1) * 2 * BE)
        for start, ref in ((to_first, x_first_ref), (to_second, x_second_ref)):
            ref[there] = cells_ref[pl.ds(pl.multiple_of(base + start * BE, BE), 2 * BE)]
        for start, ref in ((to_inner, y_inner_ref), (to_outer, y_outer_ref)):
            for layer in range(2):
                row = (2 * k + layer) * BE
                ref[row : row + BE] = cells_ref[pl.ds(base + start + layer, BE, stride=BE)]
    send_half(whole_ref, y_inner_ref, y_outer_ref, SIDE, odd)
    leaving.wait()


def send_half(source, inner_ref, outer_ref, base, odd):
    to_inner = jnp.where(odd, 0, REACH)
    to_outer = jnp.where(odd, REACH, 0)
    for row in range(FIELDS * TILES):
        there = slice(base + row * REACH, base + (row + 1) * REACH)
        inner_ref[there] = source[pl.ds(row * ROWS + to_inner, REACH)]
        outer_ref[there] = source[pl.ds(row * ROWS + to_outer, REACH)]


def change_kernel(
    cells_ref,
    x_first_ref,
    x_second_ref,
    y_inner_ref,
    y_outer_ref,
    own_ref,
    inner_ref,
    outer_ref,
    line_ref,
    right_ref,
    face_ref,
):
    device = device_index()
    odd_row = (device // GY) % 2 == 1
    odd = device % 2 == 1
    fields = range(FIELDS)

    def cell(x, k):
        return cells_ref[(k * BE + x) * BE : (k * BE + x + 1) * BE]

    def halo(first, second, k, layer, flag):
        rows = slice((2 * k + layer) * BE, (2 * k + layer + 1) * BE)
        return jnp.where(flag, first[rows], second[rows])

    def padded(x, k, y):
        return slice((k * BE + x) * PITCH + y + 1, (k * BE + x) * PITCH + y + 1 + BE)

    def all_x(k, y):
        return pl.ds(k * BE * PITCH + y + 1, BE, stride=PITCH)

    def column(x):
        if x < 0:
            return [halo(x_first_ref, x_second_ref, k, x + 2, odd_row) for k in fields]
        if x >= BE:
            return [halo(x_second_ref, x_first_ref, k, x - BE, odd_row) for k in fields]
        return [cell(x, k) for k in fields]

    total = [None] * BE
    here, up = column(-2), column(-1)
    ahead = [up[k] - here[k] for k in fields]
    left = last_face = None
    for x in range(-1, BE + 1):
        here, up, behind = up, column(x + 1), ahead
        ahead = [up[k] - here[k] for k in fields]
        half = [half_minmod(behind[k], ahead[k]) for k in fields]
        if left is not None:
            face = twice_face_flux(left, [here[k] - half[k] for k in fields], 0)
            if last_face is not None:
                total[x - 1] = [face[k] - last_face[k] for k in fields]
            last_face = face
        left = [here[k] + half[k] for k in fields]

    low_left, low_right = [], []
    for k in fields:
        far = halo(y_inner_ref, y_outer_ref, k, 0, odd)
        near = halo(y_inner_ref, y_outer_ref, k, 1, odd)
        edge = cells_ref[pl.ds(k * BE * BE, BE, stride=BE)]
        after = cells_ref[pl.ds(k * BE * BE + 1, BE, stride=BE)]
        low_left.append(near + half_minmod(near - far, edge - near))
        low_right.append(edge - half_minmod(edge - near, after - edge))
        line_ref[all_x(k, -1)] = near
        near = halo(y_outer_ref, y_inner_ref, k, 0, odd)
        far = halo(y_outer_ref, y_inner_ref, k, 1, odd)
        edge = cells_ref[pl.ds(k * BE * BE + BE - 1, BE, stride=BE)]
        line_ref[all_x(k, BE)] = near
        right_ref[all_x(k, BE)] = near - half_minmod(near - edge, far - near)
    for k, value in enumerate(twice_face_flux(low_left, low_right, 1)):
        face_ref[all_x(k, -1)] = value
    for x in range(BE):
        for k in fields:
            line_ref[padded(x, k, 0)] = cell(x, k)
    for x in range(BE):
        state = [cell(x, k) for k in fields]
        left = []
        for k in fields:
            half = half_minmod(
                state[k] - line_ref[padded(x, k, -1)], line_ref[padded(x, k, 1)] - state[k]
            )
            left.append(state[k] + half)
            right_ref[padded(x, k, 0)] = state[k] - half
        face = twice_face_flux(left, [right_ref[padded(x, k, 1)] for k in fields], 1)
        for k in fields:
            face_ref[padded(x, k, 0)] = face[k]
        for k in fields:
            total[x][k] = total[x][k] + (face[k] - face_ref[padded(x, k, -1)])

        left, right = [], []
        for k in fields:
            ahead = roll(state[k], -1) - state[k]
            half = half_minmod(roll(ahead, 1), ahead)
            left.append(state[k] + half)
            right.append(roll(state[k] - half, -1))
        face = twice_face_flux(left, right, 2)
        for k in fields:
            total[x][k] = total[x][k] + (face[k] - roll(face[k], 1))

    for k in fields:
        for tile in range(TILES):
            base = (k * TILES + tile) * ROWS
            halves = turn(total[2 * tile][k], total[2 * tile + 1][k])
            own_ref[base : base + 8], own_ref[base + 8 : base + 16] = halves
    send_half(own_ref, inner_ref, outer_ref, 0, odd)


def place_kernel(
    fastest_ref,
    whole_ref,
    change_ref,
    whole_inner_ref,
    whole_outer_ref,
    inner_ref,
    outer_ref,
    owner_ref,
    out_ref,
    held_ref,
    ready_ref,
    left,
):
    device = device_index()
    odd = device % 2 == 1
    owners = owner_ref[...]
    first = jnp.sum((owners < device).astype(jnp.int32)) - (device * BLOCKS - REACH)
    count = jnp.sum((owners == device).astype(jnp.int32))
    first = jnp.clip(first, 0, BLOCKS) + 2
    scale = (0.5 * COURANT) / jnp.max(fastest_ref[...])
    live = lax.broadcasted_iota(jnp.int32, (CAP, LANES), 0) < count
    for row in range(FIELDS * TILES):
        there = slice(row * REACH, (row + 1) * REACH)
        sent = slice(SIDE + row * REACH, SIDE + (row + 1) * REACH)
        inner = whole_inner_ref[sent] - scale * inner_ref[there]
        outer = whole_outer_ref[sent] - scale * outer_ref[there]
        base = row * HELD
        held_ref[base + 8 : base + 8 + ROWS] = (
            whole_ref[rows_of(row)] - scale * change_ref[rows_of(row)]
        )
        held_ref[base + 2 : base + 8] = jnp.where(odd, inner, outer)
        held_ref[base + 20 : base + 26] = jnp.where(odd, outer, inner)
    copies = []
    for row in range(FIELDS * TILES):
        k, tile = divmod(row, TILES)
        value = held_ref[pl.ds(row * HELD + first, CAP)]
        ready_ref[k, :, tile * LANES : (tile + 1) * LANES] = jnp.where(live, value, 0.0)
        if (row + 1) % (2 * TILES) == 0:
            two = pl.ds(k - 1, 2)
            copies.append(
                pltpu.make_async_copy(ready_ref.at[two], out_ref.at[two], left.at[k // 2])
            )
            copies[-1].start()
    for copy in copies:
        copy.wait()


HBM = pl.BlockSpec(memory_space=pltpu.HBM)
VMEM = pl.BlockSpec(memory_space=pltpu.VMEM)


def call(kernel, ins, outs, flops, scratch=()):
    return pl.pallas_call(
        kernel,
        out_shape=[
            jax.ShapeDtypeStruct(out if isinstance(out, tuple) else (out, LANES), jnp.float32)
            for out, _ in outs
        ],
        in_specs=list(ins),
        out_specs=[place for _, place in outs],
        scratch_shapes=list(scratch),
        cost_estimate=pl.CostEstimate(flops=flops, bytes_accessed=flops // 8, transcendentals=0),
        compiler_params=pltpu.CompilerParams(vmem_limit_bytes=8 * 2**20),
    )


def room(rows):
    return pltpu.VMEM((rows, LANES), jnp.float32)


def swap(value, partner, devices):
    pairs = [(i, partner(i) % devices) for i in range(devices) if partner(i) is not None]
    return lax.ppermute(value, AXES, pairs)


def per_device(ranks, prim, new_owner, new_slot):
    del new_slot
    devices = lax.axis_size(AXES)
    raw = prim.reshape(FIELDS, BLOCKS, TILES, LANES).transpose(1, 2, 0, 3).reshape(-1, LANES)
    half = FIELDS * TILES * REACH
    whole = FIELDS * TILES * ROWS
    x_first, x_second, y_inner, y_outer, fastest, cells, conserved_own = call(
        prepare_kernel,
        [HBM],
        [
            (SIDE, VMEM),
            (SIDE, VMEM),
            (SIDE + half, VMEM),
            (SIDE + half, VMEM),
            (devices, HBM),
            (FIELDS * BE * BE, VMEM),
            (whole, VMEM),
        ],
        10**6,
        [
            room(FIELDS * TILES * BLOCKS),
            room(TILES * ROWS * APART),
            room(devices),
            pltpu.SemaphoreType.DMA((CHUNKS,)),
            pltpu.SemaphoreType.DMA,
        ],
    )(pltpu.with_memory_space_constraint(raw, pltpu.HBM))
    everyone = lax.all_to_all(fastest, AXES, 0, 0, tiled=True)

    def within(i, j):
        return j if 0 <= j < devices and i // ranks == j // ranks else None

    x_first = swap(x_first, lambda i: i + GY if (i // GY) % 2 == 0 else i - GY, devices)
    x_second = swap(x_second, lambda i: i + GY if (i // GY) % 2 == 1 else i - GY, devices)
    y_outer = swap(y_outer, lambda i: i + 1 if i % 2 == 1 else i - 1, devices)
    y_inner = swap(y_inner, lambda i: i ^ 1, devices)
    own, to_inner, to_outer = call(
        change_kernel,
        [VMEM] * 5,
        [(whole, VMEM), (half, VMEM), (half, VMEM)],
        2 * 10**7,
        [room(FIELDS * BE * PITCH)] * 3,
    )(cells, x_first, x_second, y_inner, y_outer)
    from_outer = swap(to_outer, lambda i: within(i, i + 1 if i % 2 == 1 else i - 1), devices)
    from_inner = swap(to_inner, lambda i: i ^ 1, devices)
    (placed,) = call(
        place_kernel,
        [VMEM] * 8,
        [((FIELDS, CAP, TILES * LANES), HBM)],
        10**6,
        [
            room(FIELDS * TILES * HELD),
            pltpu.VMEM((FIELDS, CAP, TILES * LANES), jnp.float32),
            pltpu.SemaphoreType.DMA((FIELDS // 2,)),
        ],
    )(
        everyone,
        conserved_own,
        own,
        y_inner,
        y_outer,
        from_inner,
        from_outer,
        new_owner.reshape(-1, LANES),
    )
    return placed


def solution(mesh):
    return jax.shard_map(
        functools.partial(per_device, mesh.shape["inner"]),
        mesh=mesh,
        in_specs=(P(None, AXES, None), P(), P()),
        out_specs=P(None, AXES, None),
        check_vma=False,
    )
```

```python
import functools

import jax
import jax.numpy as jnp
from jax import lax
from jax.experimental import pallas as pl
from jax.experimental.pallas import tpu as pltpu
from jax.sharding import PartitionSpec as P


BE = 8
GY = 16
AXES = ("outer", "inner")
GAMMA = 5.0 / 3.0
COURANT = 0.8
LANES = 128
TILES = 4
FIELDS = 8
BLOCKS = 12
REACH = 6
CAP = 24
ROWS = 16
HELD = 40
SIDE = FIELDS * 2 * BE
HALF = FIELDS * TILES * REACH
PITCH = BE + 2
APART = FIELDS + 1
CHUNKS = 4


def roll(value, shift):
    return pltpu.roll(value, shift % LANES, 1)


def half_minmod(former, latter):
    return 0.5 * (
        jnp.maximum(jnp.minimum(former, latter), 0.0)
        + jnp.minimum(jnp.maximum(former, latter), 0.0)
    )


def sound(density, pressure, field_sq):
    pushed = GAMMA * pressure + field_sq
    return pushed * lax.rsqrt(pushed * density)


def squared(state):
    return state[5] * state[5] + state[6] * state[6] + state[7] * state[7]


def conserved(state, field_sq):
    density, pressure = state[0], state[4]
    momentum = [density * state[1 + k] for k in range(3)]
    kinetic = momentum[0] * state[1] + momentum[1] * state[2] + momentum[2] * state[3]
    energy = pressure * (1.0 / (GAMMA - 1.0)) + 0.5 * (kinetic + field_sq)
    return [density, *momentum, energy, state[5], state[6], state[7]]


def flux_parts(state, normal):
    field_sq = squared(state)
    total_pressure = state[4] + 0.5 * field_sq
    whole = conserved(state, field_sq)
    speed, field = state[1 + normal], state[5 + normal]
    along = state[1] * state[5] + state[2] * state[6] + state[3] * state[7]
    momentum = [whole[1 + k] * speed - state[5 + k] * field for k in range(3)]
    momentum[normal] = momentum[normal] + total_pressure
    induction = [
        None if k == normal else state[5 + k] * speed - state[1 + k] * field for k in range(3)
    ]
    energy = (whole[4] + total_pressure) * speed - field * along
    signal = jnp.abs(speed) + sound(state[0], state[4], field_sq)
    return [whole[1 + normal], *momentum, energy, *induction], signal, whole


def twice_face_flux(left, right, normal):
    flux_left, signal_left, whole_left = flux_parts(left, normal)
    flux_right, signal_right, whole_right = flux_parts(right, normal)
    fastest = jnp.maximum(signal_left, signal_right)
    result = []
    for k in range(FIELDS):
        spread = fastest * (whole_right[k] - whole_left[k])
        result.append(-spread if flux_left[k] is None else flux_left[k] + flux_right[k] - spread)
    return result


def rows_of(index):
    return slice(index * ROWS, (index + 1) * ROWS)


def device_index():
    return lax.axis_index(AXES[0]) * lax.axis_size(AXES[1]) + lax.axis_index(AXES[1])


def turn(first, second):
    row = lax.broadcasted_iota(jnp.int32, (8, LANES), 0)
    group = lax.broadcasted_iota(jnp.int32, (8, LANES), 1) // 8

    def skewed(value, shift):
        return pltpu.roll(value, shift, 1, stride=8, stride_axis=0)

    def across(value, source):
        return jnp.take_along_axis(value, source, axis=0, mode="promise_in_bounds")

    first, second = skewed(first, 0), skewed(second, 64)

    def picked(index):
        source = (row + group + index) & 15
        return jnp.where(source < 8, across(first, source & 7), across(second, source & 7))

    upper, lower = skewed(picked(1), 8), skewed(picked(9), 72)
    return across(lower, 7 - row), across(upper, 7 - row)


def prepare_kernel(
    prim_ref,
    x_first_ref,
    x_second_ref,
    y_inner_ref,
    y_outer_ref,
    fastest_ref,
    cells_ref,
    whole_ref,
    raw_ref,
    spread_ref,
    filled_ref,
    arrived,
    left,
):
    device = device_index()
    odd_row = (device // GY) % 2 == 1
    odd = device % 2 == 1
    part = TILES * FIELDS * BLOCKS // CHUNKS
    copies = [
        pltpu.make_async_copy(
            prim_ref.at[pl.ds(i * part, part)], raw_ref.at[pl.ds(i * part, part)], arrived.at[i]
        )
        for i in range(CHUNKS)
    ]
    for copy in copies:
        copy.start()
    for block in range(BLOCKS):
        if block % (BLOCKS // CHUNKS) == 0:
            copies[block // (BLOCKS // CHUNKS)].wait()
        rows = [block]
        if block == 0:
            rows += [12, 13, 14]
        if block == BLOCKS - 1:
            rows += [15]
        for tile in range(TILES):
            value = raw_ref[(block * TILES + tile) * FIELDS : (block * TILES + tile + 1) * FIELDS]
            for row in rows:
                base = (tile * ROWS + row) * APART
                spread_ref[base : base + FIELDS] = value

    def cell(k, tile, half):
        return spread_ref[pl.ds((tile * ROWS + 8 * half) * APART + k, 8, stride=APART)]

    best = None
    for tile in range(TILES):
        for half in range(2):
            state = [cell(k, tile, half) for k in range(FIELDS)]
            field_sq = squared(state)
            speed = (
                jnp.abs(state[1])
                + jnp.abs(state[2])
                + jnp.abs(state[3])
                + 3.0 * sound(state[0], state[4], field_sq)
            )
            best = speed if best is None else jnp.maximum(best, speed)
            for k, value in enumerate(conserved(state, field_sq)):
                base = (k * TILES + tile) * ROWS + 8 * half
                whole_ref[base : base + 8] = value
    filled_ref[...] = jnp.broadcast_to(jnp.max(best, keepdims=True), filled_ref.shape)
    leaving = pltpu.make_async_copy(filled_ref, fastest_ref, left)
    leaving.start()
    for k in range(FIELDS):
        for tile in range(TILES):
            halves = turn(cell(k, tile, 0), cell(k, tile, 1))
            base = (k * BE + 2 * tile) * BE
            cells_ref[base : base + 8], cells_ref[base + 8 : base + 16] = halves
    to_first = jnp.where(odd_row, 0, BE - 2)
    to_second = jnp.where(odd_row, BE - 2, 0)
    to_inner = jnp.where(odd, 0, BE - 2)
    to_outer = jnp.where(odd, BE - 2, 0)
    for k in range(FIELDS):
        base, there = k * BE * BE, slice(k * 2 * BE, (k + 1) * 2 * BE)
        for start, ref in ((to_first, x_first_ref), (to_second, x_second_ref)):
            ref[there] = cells_ref[pl.ds(pl.multiple_of(base + start * BE, BE), 2 * BE)]
        for start, ref in ((to_inner, y_inner_ref), (to_outer, y_outer_ref)):
            for layer in range(2):
                row = (2 * k + layer) * BE
                ref[row : row + BE] = cells_ref[pl.ds(base + start + layer, BE, stride=BE)]
    leaving.wait()


def send_half(source, inner_ref, outer_ref, base, odd):
    to_inner = jnp.where(odd, 0, REACH)
    to_outer = jnp.where(odd, REACH, 0)
    for row in range(FIELDS * TILES):
        there = slice(base + row * REACH, base + (row + 1) * REACH)
        inner_ref[there] = source[pl.ds(row * ROWS + to_inner, REACH)]
        outer_ref[there] = source[pl.ds(row * ROWS + to_outer, REACH)]


def change_kernel(
    cells_ref,
    whole_ref,
    x_first_ref,
    x_second_ref,
    y_inner_ref,
    y_outer_ref,
    own_ref,
    inner_ref,
    outer_ref,
    line_ref,
    right_ref,
    face_ref,
):
    device = device_index()
    odd_row = (device // GY) % 2 == 1
    odd = device % 2 == 1
    fields = range(FIELDS)

    def cell(x, k):
        return cells_ref[(k * BE + x) * BE : (k * BE + x + 1) * BE]

    def halo(first, second, k, layer, flag):
        rows = slice((2 * k + layer) * BE, (2 * k + layer + 1) * BE)
        return jnp.where(flag, first[rows], second[rows])

    def padded(x, k, y):
        return slice((k * BE + x) * PITCH + y + 1, (k * BE + x) * PITCH + y + 1 + BE)

    def all_x(k, y):
        return pl.ds(k * BE * PITCH + y + 1, BE, stride=PITCH)

    def column(x):
        if x < 0:
            return [halo(x_first_ref, x_second_ref, k, x + 2, odd_row) for k in fields]
        if x >= BE:
            return [halo(x_second_ref, x_first_ref, k, x - BE, odd_row) for k in fields]
        return [cell(x, k) for k in fields]

    total = [None] * BE
    here, up = column(-2), column(-1)
    ahead = [up[k] - here[k] for k in fields]
    left = last_face = None
    for x in range(-1, BE + 1):
        here, up, behind = up, column(x + 1), ahead
        ahead = [up[k] - here[k] for k in fields]
        half = [half_minmod(behind[k], ahead[k]) for k in fields]
        if left is not None:
            face = twice_face_flux(left, [here[k] - half[k] for k in fields], 0)
            if last_face is not None:
                total[x - 1] = [face[k] - last_face[k] for k in fields]
            last_face = face
        left = [here[k] + half[k] for k in fields]

    low_left, low_right = [], []
    for k in fields:
        far = halo(y_inner_ref, y_outer_ref, k, 0, odd)
        near = halo(y_inner_ref, y_outer_ref, k, 1, odd)
        edge = cells_ref[pl.ds(k * BE * BE, BE, stride=BE)]
        after = cells_ref[pl.ds(k * BE * BE + 1, BE, stride=BE)]
        low_left.append(near + half_minmod(near - far, edge - near))
        low_right.append(edge - half_minmod(edge - near, after - edge))
        line_ref[all_x(k, -1)] = near
        near = halo(y_outer_ref, y_inner_ref, k, 0, odd)
        far = halo(y_outer_ref, y_inner_ref, k, 1, odd)
        edge = cells_ref[pl.ds(k * BE * BE + BE - 1, BE, stride=BE)]
        line_ref[all_x(k, BE)] = near
        right_ref[all_x(k, BE)] = near - half_minmod(near - edge, far - near)
    for k, value in enumerate(twice_face_flux(low_left, low_right, 1)):
        face_ref[all_x(k, -1)] = value
    for x in range(BE):
        for k in fields:
            line_ref[padded(x, k, 0)] = cell(x, k)
    for x in range(BE):
        state = [cell(x, k) for k in fields]
        left = []
        for k in fields:
            half = half_minmod(
                state[k] - line_ref[padded(x, k, -1)], line_ref[padded(x, k, 1)] - state[k]
            )
            left.append(state[k] + half)
            right_ref[padded(x, k, 0)] = state[k] - half
        face = twice_face_flux(left, [right_ref[padded(x, k, 1)] for k in fields], 1)
        for k in fields:
            face_ref[padded(x, k, 0)] = face[k]
        for k in fields:
            total[x][k] = total[x][k] + (face[k] - face_ref[padded(x, k, -1)])

        left, right = [], []
        for k in fields:
            ahead = roll(state[k], -1) - state[k]
            half = half_minmod(roll(ahead, 1), ahead)
            left.append(state[k] + half)
            right.append(roll(state[k] - half, -1))
        face = twice_face_flux(left, right, 2)
        for k in fields:
            total[x][k] = total[x][k] + (face[k] - roll(face[k], 1))

    for k in fields:
        for tile in range(TILES):
            base = (k * TILES + tile) * ROWS
            halves = turn(total[2 * tile][k], total[2 * tile + 1][k])
            own_ref[base : base + 8], own_ref[base + 8 : base + 16] = halves
    send_half(whole_ref, inner_ref, outer_ref, 0, odd)
    send_half(own_ref, inner_ref, outer_ref, HALF, odd)


def place_kernel(
    fastest_ref,
    whole_ref,
    change_ref,
    inner_ref,
    outer_ref,
    owner_ref,
    out_ref,
    held_ref,
    ready_ref,
    left,
):
    device = device_index()
    odd = device % 2 == 1
    owners = owner_ref[...]
    first = jnp.sum((owners < device).astype(jnp.int32)) - (device * BLOCKS - REACH)
    count = jnp.sum((owners == device).astype(jnp.int32))
    first = jnp.clip(first, 0, BLOCKS) + 2
    scale = (0.5 * COURANT) / jnp.max(fastest_ref[...])
    live = lax.broadcasted_iota(jnp.int32, (CAP, LANES), 0) < count
    for row in range(FIELDS * TILES):
        there = slice(row * REACH, (row + 1) * REACH)
        later = slice(HALF + row * REACH, HALF + (row + 1) * REACH)
        inner = inner_ref[there] - scale * inner_ref[later]
        outer = outer_ref[there] - scale * outer_ref[later]
        base = row * HELD
        held_ref[base + 8 : base + 8 + ROWS] = (
            whole_ref[rows_of(row)] - scale * change_ref[rows_of(row)]
        )
        held_ref[base + 2 : base + 8] = jnp.where(odd, inner, outer)
        held_ref[base + 20 : base + 26] = jnp.where(odd, outer, inner)
    copies = []
    for row in range(FIELDS * TILES):
        k, tile = divmod(row, TILES)
        value = held_ref[pl.ds(row * HELD + first, CAP)]
        ready_ref[k, :, tile * LANES : (tile + 1) * LANES] = jnp.where(live, value, 0.0)
        if (row + 1) % (2 * TILES) == 0:
            two = pl.ds(k - 1, 2)
            copies.append(
                pltpu.make_async_copy(ready_ref.at[two], out_ref.at[two], left.at[k // 2])
            )
            copies[-1].start()
    for copy in copies:
        copy.wait()


HBM = pl.BlockSpec(memory_space=pltpu.HBM)
VMEM = pl.BlockSpec(memory_space=pltpu.VMEM)


def call(kernel, ins, outs, flops, scratch=()):
    return pl.pallas_call(
        kernel,
        out_shape=[
            jax.ShapeDtypeStruct(out if isinstance(out, tuple) else (out, LANES), jnp.float32)
            for out, _ in outs
        ],
        in_specs=list(ins),
        out_specs=[place for _, place in outs],
        scratch_shapes=list(scratch),
        cost_estimate=pl.CostEstimate(flops=flops, bytes_accessed=flops // 8, transcendentals=0),
        compiler_params=pltpu.CompilerParams(vmem_limit_bytes=8 * 2**20),
    )


def room(rows):
    return pltpu.VMEM((rows, LANES), jnp.float32)


def swap(value, partner, devices):
    pairs = [(i, partner(i) % devices) for i in range(devices) if partner(i) is not None]
    return lax.ppermute(value, AXES, pairs)


def per_device(ranks, prim, new_owner, new_slot):
    del new_slot
    devices = lax.axis_size(AXES)
    raw = prim.reshape(FIELDS, BLOCKS, TILES, LANES).transpose(1, 2, 0, 3).reshape(-1, LANES)
    whole = FIELDS * TILES * ROWS
    x_first, x_second, y_inner, y_outer, fastest, cells, conserved_own = call(
        prepare_kernel,
        [HBM],
        [
            (SIDE, VMEM),
            (SIDE, VMEM),
            (SIDE, VMEM),
            (SIDE, VMEM),
            (devices, HBM),
            (FIELDS * BE * BE, VMEM),
            (whole, VMEM),
        ],
        10**6,
        [
            room(FIELDS * TILES * BLOCKS),
            room(TILES * ROWS * APART),
            room(devices),
            pltpu.SemaphoreType.DMA((CHUNKS,)),
            pltpu.SemaphoreType.DMA,
        ],
    )(pltpu.with_memory_space_constraint(raw, pltpu.HBM))
    everyone = lax.all_to_all(fastest, AXES, 0, 0, tiled=True)

    def within(i, j):
        return j if 0 <= j < devices and i // ranks == j // ranks else None

    x_first = swap(x_first, lambda i: i + GY if (i // GY) % 2 == 0 else i - GY, devices)
    x_second = swap(x_second, lambda i: i + GY if (i // GY) % 2 == 1 else i - GY, devices)
    y_outer = swap(y_outer, lambda i: i + 1 if i % 2 == 1 else i - 1, devices)
    y_inner = swap(y_inner, lambda i: i ^ 1, devices)
    own, to_inner, to_outer = call(
        change_kernel,
        [VMEM] * 6,
        [(whole, VMEM), (2 * HALF, VMEM), (2 * HALF, VMEM)],
        2 * 10**7,
        [room(FIELDS * BE * PITCH)] * 3,
    )(cells, conserved_own, x_first, x_second, y_inner, y_outer)
    from_outer = swap(to_outer, lambda i: within(i, i + 1 if i % 2 == 1 else i - 1), devices)
    from_inner = swap(to_inner, lambda i: i ^ 1, devices)
    (placed,) = call(
        place_kernel,
        [VMEM] * 6,
        [((FIELDS, CAP, TILES * LANES), HBM)],
        10**6,
        [
            room(FIELDS * TILES * HELD),
            pltpu.VMEM((FIELDS, CAP, TILES * LANES), jnp.float32),
            pltpu.SemaphoreType.DMA((FIELDS // 2,)),
        ],
    )(
        everyone,
        conserved_own,
        own,
        from_inner,
        from_outer,
        new_owner.reshape(-1, LANES),
    )
    return placed


def solution(mesh):
    return jax.shard_map(
        functools.partial(per_device, mesh.shape["inner"]),
        mesh=mesh,
        in_specs=(P(None, AXES, None), P(), P()),
        out_specs=P(None, AXES, None),
        check_vma=False,
    )
```

```python
import functools

import jax
import jax.numpy as jnp
from jax import lax
from jax.experimental import pallas as pl
from jax.experimental.pallas import tpu as pltpu
from jax.sharding import PartitionSpec as P


BE = 8
GY = 16
AXES = ("outer", "inner")
GAMMA = 5.0 / 3.0
COURANT = 0.8
LANES = 128
TILES = 4
FIELDS = 8
BLOCKS = 12
REACH = 6
CAP = 24
ROWS = 16
HELD = 40
SIDE = FIELDS * 2 * BE
PITCH = BE + 2
APART = FIELDS + 1
CHUNKS = 4


def roll(value, shift):
    return pltpu.roll(value, shift % LANES, 1)


def half_minmod(former, latter):
    return 0.5 * (
        jnp.maximum(jnp.minimum(former, latter), 0.0)
        + jnp.minimum(jnp.maximum(former, latter), 0.0)
    )


def sound(density, pressure, field_sq):
    pushed = GAMMA * pressure + field_sq
    return pushed * lax.rsqrt(pushed * density)


def squared(state):
    return state[5] * state[5] + state[6] * state[6] + state[7] * state[7]


def conserved(state, field_sq):
    density, pressure = state[0], state[4]
    momentum = [density * state[1 + k] for k in range(3)]
    kinetic = momentum[0] * state[1] + momentum[1] * state[2] + momentum[2] * state[3]
    energy = pressure * (1.0 / (GAMMA - 1.0)) + 0.5 * (kinetic + field_sq)
    return [density, *momentum, energy, state[5], state[6], state[7]]


def flux_parts(state, normal):
    field_sq = squared(state)
    total_pressure = state[4] + 0.5 * field_sq
    whole = conserved(state, field_sq)
    speed, field = state[1 + normal], state[5 + normal]
    along = state[1] * state[5] + state[2] * state[6] + state[3] * state[7]
    momentum = [whole[1 + k] * speed - state[5 + k] * field for k in range(3)]
    momentum[normal] = momentum[normal] + total_pressure
    induction = [
        None if k == normal else state[5 + k] * speed - state[1 + k] * field for k in range(3)
    ]
    energy = (whole[4] + total_pressure) * speed - field * along
    signal = jnp.abs(speed) + sound(state[0], state[4], field_sq)
    return [whole[1 + normal], *momentum, energy, *induction], signal, whole


def twice_face_flux(left, right, normal):
    flux_left, signal_left, whole_left = flux_parts(left, normal)
    flux_right, signal_right, whole_right = flux_parts(right, normal)
    fastest = jnp.maximum(signal_left, signal_right)
    result = []
    for k in range(FIELDS):
        spread = fastest * (whole_right[k] - whole_left[k])
        result.append(-spread if flux_left[k] is None else flux_left[k] + flux_right[k] - spread)
    return result


def rows_of(index):
    return slice(index * ROWS, (index + 1) * ROWS)


def device_index():
    return lax.axis_index(AXES[0]) * lax.axis_size(AXES[1]) + lax.axis_index(AXES[1])


def turn(first, second):
    row = lax.broadcasted_iota(jnp.int32, (8, LANES), 0)
    group = lax.broadcasted_iota(jnp.int32, (8, LANES), 1) // 8

    def skewed(value, shift):
        return pltpu.roll(value, shift, 1, stride=8, stride_axis=0)

    def across(value, source):
        return jnp.take_along_axis(value, source, axis=0, mode="promise_in_bounds")

    first, second = skewed(first, 0), skewed(second, 64)

    def picked(index):
        source = (row + group + index) & 15
        return jnp.where(source < 8, across(first, source & 7), across(second, source & 7))

    upper, lower = skewed(picked(1), 8), skewed(picked(9), 72)
    return across(lower, 7 - row), across(upper, 7 - row)


def prepare_kernel(
    prim_ref,
    x_first_ref,
    x_second_ref,
    y_inner_ref,
    y_outer_ref,
    fastest_ref,
    cells_ref,
    whole_ref,
    raw_ref,
    spread_ref,
    filled_ref,
    arrived,
    left,
):
    device = device_index()
    odd_row = (device // GY) % 2 == 1
    odd = device % 2 == 1
    part = TILES * FIELDS * BLOCKS // CHUNKS
    copies = [
        pltpu.make_async_copy(
            prim_ref.at[pl.ds(i * part, part)], raw_ref.at[pl.ds(i * part, part)], arrived.at[i]
        )
        for i in range(CHUNKS)
    ]
    for copy in copies:
        copy.start()
    for block in range(BLOCKS):
        if block % (BLOCKS // CHUNKS) == 0:
            copies[block // (BLOCKS // CHUNKS)].wait()
        rows = [block]
        if block == 0:
            rows += [12, 13, 14]
        if block == BLOCKS - 1:
            rows += [15]
        for tile in range(TILES):
            value = raw_ref[(block * TILES + tile) * FIELDS : (block * TILES + tile + 1) * FIELDS]
            for row in rows:
                base = (tile * ROWS + row) * APART
                spread_ref[base : base + FIELDS] = value

    def cell(k, tile, half):
        return spread_ref[pl.ds((tile * ROWS + 8 * half) * APART + k, 8, stride=APART)]

    best = None
    for tile in range(TILES):
        for half in range(2):
            state = [cell(k, tile, half) for k in range(FIELDS)]
            speed = (
                jnp.abs(state[1])
                + jnp.abs(state[2])
                + jnp.abs(state[3])
                + 3.0 * sound(state[0], state[4], squared(state))
            )
            best = speed if best is None else jnp.maximum(best, speed)
    filled_ref[...] = jnp.broadcast_to(jnp.max(best, keepdims=True), filled_ref.shape)
    leaving = pltpu.make_async_copy(filled_ref, fastest_ref, left)
    leaving.start()
    for tile in range(TILES):
        for half in range(2):
            state = [cell(k, tile, half) for k in range(FIELDS)]
            for k, value in enumerate(conserved(state, squared(state))):
                base = (k * TILES + tile) * ROWS + 8 * half
                whole_ref[base : base + 8] = value
    for k in range(FIELDS):
        for tile in range(TILES):
            halves = turn(cell(k, tile, 0), cell(k, tile, 1))
            base = (k * BE + 2 * tile) * BE
            cells_ref[base : base + 8], cells_ref[base + 8 : base + 16] = halves
    to_first = jnp.where(odd_row, 0, BE - 2)
    to_second = jnp.where(odd_row, BE - 2, 0)
    to_inner = jnp.where(odd, 0, BE - 2)
    to_outer = jnp.where(odd, BE - 2, 0)
    for k in range(FIELDS):
        base, there = k * BE * BE, slice(k * 2 * BE, (k + 1) * 2 * BE)
        for start, ref in ((to_first, x_first_ref), (to_second, x_second_ref)):
            ref[there] = cells_ref[pl.ds(pl.multiple_of(base + start * BE, BE), 2 * BE)]
        for start, ref in ((to_inner, y_inner_ref), (to_outer, y_outer_ref)):
            for layer in range(2):
                row = (2 * k + layer) * BE
                ref[row : row + BE] = cells_ref[pl.ds(base + start + layer, BE, stride=BE)]
    send_half(whole_ref, y_inner_ref, y_outer_ref, SIDE, odd)
    leaving.wait()


def send_half(source, inner_ref, outer_ref, base, odd):
    to_inner = jnp.where(odd, 0, REACH)
    to_outer = jnp.where(odd, REACH, 0)
    for row in range(FIELDS * TILES):
        there = slice(base + row * REACH, base + (row + 1) * REACH)
        inner_ref[there] = source[pl.ds(row * ROWS + to_inner, REACH)]
        outer_ref[there] = source[pl.ds(row * ROWS + to_outer, REACH)]


def change_kernel(
    cells_ref,
    x_first_ref,
    x_second_ref,
    y_inner_ref,
    y_outer_ref,
    own_ref,
    inner_ref,
    outer_ref,
    line_ref,
    right_ref,
    face_ref,
):
    device = device_index()
    odd_row = (device // GY) % 2 == 1
    odd = device % 2 == 1
    fields = range(FIELDS)

    def cell(x, k):
        return cells_ref[(k * BE + x) * BE : (k * BE + x + 1) * BE]

    def halo(first, second, k, layer, flag):
        rows = slice((2 * k + layer) * BE, (2 * k + layer + 1) * BE)
        return jnp.where(flag, first[rows], second[rows])

    def padded(x, k, y):
        return slice((k * BE + x) * PITCH + y + 1, (k * BE + x) * PITCH + y + 1 + BE)

    def all_x(k, y):
        return pl.ds(k * BE * PITCH + y + 1, BE, stride=PITCH)

    def column(x):
        if x < 0:
            return [halo(x_first_ref, x_second_ref, k, x + 2, odd_row) for k in fields]
        if x >= BE:
            return [halo(x_second_ref, x_first_ref, k, x - BE, odd_row) for k in fields]
        return [cell(x, k) for k in fields]

    total = [None] * BE
    here, up = column(-2), column(-1)
    ahead = [up[k] - here[k] for k in fields]
    left = last_face = None
    for x in range(-1, BE + 1):
        here, up, behind = up, column(x + 1), ahead
        ahead = [up[k] - here[k] for k in fields]
        half = [half_minmod(behind[k], ahead[k]) for k in fields]
        if left is not None:
            face = twice_face_flux(left, [here[k] - half[k] for k in fields], 0)
            if last_face is not None:
                total[x - 1] = [face[k] - last_face[k] for k in fields]
            last_face = face
        left = [here[k] + half[k] for k in fields]

    low_left, low_right = [], []
    for k in fields:
        far = halo(y_inner_ref, y_outer_ref, k, 0, odd)
        near = halo(y_inner_ref, y_outer_ref, k, 1, odd)
        edge = cells_ref[pl.ds(k * BE * BE, BE, stride=BE)]
        after = cells_ref[pl.ds(k * BE * BE + 1, BE, stride=BE)]
        low_left.append(near + half_minmod(near - far, edge - near))
        low_right.append(edge - half_minmod(edge - near, after - edge))
        line_ref[all_x(k, -1)] = near
        near = halo(y_outer_ref, y_inner_ref, k, 0, odd)
        far = halo(y_outer_ref, y_inner_ref, k, 1, odd)
        edge = cells_ref[pl.ds(k * BE * BE + BE - 1, BE, stride=BE)]
        line_ref[all_x(k, BE)] = near
        right_ref[all_x(k, BE)] = near - half_minmod(near - edge, far - near)
    for k, value in enumerate(twice_face_flux(low_left, low_right, 1)):
        face_ref[all_x(k, -1)] = value
    for x in range(BE):
        for k in fields:
            line_ref[padded(x, k, 0)] = cell(x, k)
    for x in range(BE):
        state = [cell(x, k) for k in fields]
        left = []
        for k in fields:
            half = half_minmod(
                state[k] - line_ref[padded(x, k, -1)], line_ref[padded(x, k, 1)] - state[k]
            )
            left.append(state[k] + half)
            right_ref[padded(x, k, 0)] = state[k] - half
        face = twice_face_flux(left, [right_ref[padded(x, k, 1)] for k in fields], 1)
        for k in fields:
            face_ref[padded(x, k, 0)] = face[k]
        for k in fields:
            total[x][k] = total[x][k] + (face[k] - face_ref[padded(x, k, -1)])

        left, right = [], []
        for k in fields:
            ahead = roll(state[k], -1) - state[k]
            half = half_minmod(roll(ahead, 1), ahead)
            left.append(state[k] + half)
            right.append(roll(state[k] - half, -1))
        face = twice_face_flux(left, right, 2)
        for k in fields:
            total[x][k] = total[x][k] + (face[k] - roll(face[k], 1))

    for k in fields:
        for tile in range(TILES):
            base = (k * TILES + tile) * ROWS
            halves = turn(total[2 * tile][k], total[2 * tile + 1][k])
            own_ref[base : base + 8], own_ref[base + 8 : base + 16] = halves
    send_half(own_ref, inner_ref, outer_ref, 0, odd)


def place_kernel(
    fastest_ref,
    whole_ref,
    change_ref,
    whole_inner_ref,
    whole_outer_ref,
    inner_ref,
    outer_ref,
    owner_ref,
    out_ref,
    held_ref,
    ready_ref,
    left,
):
    device = device_index()
    odd = device % 2 == 1
    owners = owner_ref[...]
    first = jnp.sum((owners < device).astype(jnp.int32)) - (device * BLOCKS - REACH)
    count = jnp.sum((owners == device).astype(jnp.int32))
    first = jnp.clip(first, 0, BLOCKS) + 2
    scale = (0.5 * COURANT) / jnp.max(fastest_ref[...])
    live = lax.broadcasted_iota(jnp.int32, (CAP, LANES), 0) < count
    copies = []
    for k in range(FIELDS):
        for row in range(k * TILES, (k + 1) * TILES):
            there = slice(row * REACH, (row + 1) * REACH)
            sent = slice(SIDE + row * REACH, SIDE + (row + 1) * REACH)
            inner = whole_inner_ref[sent] - scale * inner_ref[there]
            outer = whole_outer_ref[sent] - scale * outer_ref[there]
            base = row * HELD
            held_ref[base + 8 : base + 8 + ROWS] = (
                whole_ref[rows_of(row)] - scale * change_ref[rows_of(row)]
            )
            held_ref[base + 2 : base + 8] = jnp.where(odd, inner, outer)
            held_ref[base + 20 : base + 26] = jnp.where(odd, outer, inner)
        for tile in range(TILES):
            value = held_ref[pl.ds((k * TILES + tile) * HELD + first, CAP)]
            ready_ref[k, :, tile * LANES : (tile + 1) * LANES] = jnp.where(live, value, 0.0)
        copies.append(
            pltpu.make_async_copy(ready_ref.at[pl.ds(k, 1)], out_ref.at[pl.ds(k, 1)], left.at[k])
        )
        copies[-1].start()
    for copy in copies:
        copy.wait()


HBM = pl.BlockSpec(memory_space=pltpu.HBM)
VMEM = pl.BlockSpec(memory_space=pltpu.VMEM)


def call(kernel, ins, outs, flops, scratch=()):
    return pl.pallas_call(
        kernel,
        out_shape=[
            jax.ShapeDtypeStruct(out if isinstance(out, tuple) else (out, LANES), jnp.float32)
            for out, _ in outs
        ],
        in_specs=list(ins),
        out_specs=[place for _, place in outs],
        scratch_shapes=list(scratch),
        cost_estimate=pl.CostEstimate(flops=flops, bytes_accessed=flops // 8, transcendentals=0),
        compiler_params=pltpu.CompilerParams(vmem_limit_bytes=8 * 2**20),
    )


def room(rows):
    return pltpu.VMEM((rows, LANES), jnp.float32)


def swap(value, partner, devices):
    pairs = [(i, partner(i) % devices) for i in range(devices) if partner(i) is not None]
    return lax.ppermute(value, AXES, pairs)


def per_device(ranks, prim, new_owner, new_slot):
    del new_slot
    devices = lax.axis_size(AXES)
    raw = prim.reshape(FIELDS, BLOCKS, TILES, LANES).transpose(1, 2, 0, 3).reshape(-1, LANES)
    half = FIELDS * TILES * REACH
    whole = FIELDS * TILES * ROWS
    x_first, x_second, y_inner, y_outer, fastest, cells, conserved_own = call(
        prepare_kernel,
        [HBM],
        [
            (SIDE, VMEM),
            (SIDE, VMEM),
            (SIDE + half, VMEM),
            (SIDE + half, VMEM),
            (devices, HBM),
            (FIELDS * BE * BE, VMEM),
            (whole, VMEM),
        ],
        10**6,
        [
            room(FIELDS * TILES * BLOCKS),
            room(TILES * ROWS * APART),
            room(devices),
            pltpu.SemaphoreType.DMA((CHUNKS,)),
            pltpu.SemaphoreType.DMA,
        ],
    )(pltpu.with_memory_space_constraint(raw, pltpu.HBM))
    everyone = lax.all_to_all(fastest, AXES, 0, 0, tiled=True)

    def within(i, j):
        return j if 0 <= j < devices and i // ranks == j // ranks else None

    x_first = swap(x_first, lambda i: i + GY if (i // GY) % 2 == 0 else i - GY, devices)
    x_second = swap(x_second, lambda i: i + GY if (i // GY) % 2 == 1 else i - GY, devices)
    y_outer = swap(y_outer, lambda i: i + 1 if i % 2 == 1 else i - 1, devices)
    y_inner = swap(y_inner, lambda i: i ^ 1, devices)
    own, to_inner, to_outer = call(
        change_kernel,
        [VMEM] * 5,
        [(whole, VMEM), (half, VMEM), (half, VMEM)],
        2 * 10**7,
        [room(FIELDS * BE * PITCH)] * 3,
    )(cells, x_first, x_second, y_inner, y_outer)
    from_outer = swap(to_outer, lambda i: within(i, i + 1 if i % 2 == 1 else i - 1), devices)
    from_inner = swap(to_inner, lambda i: i ^ 1, devices)
    (placed,) = call(
        place_kernel,
        [VMEM] * 8,
        [((FIELDS, CAP, TILES * LANES), HBM)],
        10**6,
        [
            room(FIELDS * TILES * HELD),
            pltpu.VMEM((FIELDS, CAP, TILES * LANES), jnp.float32),
            pltpu.SemaphoreType.DMA((FIELDS,)),
        ],
    )(
        everyone,
        conserved_own,
        own,
        y_inner,
        y_outer,
        from_inner,
        from_outer,
        new_owner.reshape(-1, LANES),
    )
    return placed


def solution(mesh):
    return jax.shard_map(
        functools.partial(per_device, mesh.shape["inner"]),
        mesh=mesh,
        in_specs=(P(None, AXES, None), P(), P()),
        out_specs=P(None, AXES, None),
        check_vma=False,
    )
```
